512 devices in a mesh: grp: 8 (over x, core), dev: 64 (over y, z).
Axes of the slice: x: 4, y: 4, z: 16, core: 2. Of those that a mesh axis runs over, the one named last changes fastest.
Arguments:
- line_bin: int32 [1048576], P(('grp', 'dev')), may hold values from 0 to 65535, as said below
- line_slot: int32 [1048576], P(('grp', 'dev')), may hold values from 0 to 31
- strength: float32 [1048576], P(('grp', 'dev')), may hold values from 0.05 to 1
- line_count: int32 [512], P(('grp', 'dev')), may hold values from 1024 to 2048
- gauss_width: float32 [32], replicated, may hold values from 2 to 40
- lorentz_width: float32 [32], replicated, may hold values from 1 to 30
- mixing: float32 [32], replicated, may hold values from 0.1 to 0.9
- profile_factor: float32 [32, 257], replicated, may hold values from 0.25 to 1.75
Outputs:
- spectrum: float32 [524288], P(('grp', 'dev'))
The draws below stay inside these ranges and needn't reach their ends.
Inputs may be any that keep to these rules, and one draw needn't show every extreme that they name: `line_bin`: every line of device (g, d) (the d-th block of 2048 lines within the g-th group of 64 blocks) has a bin within (d - 2) * 1024 to (d + 3) * 1024 - 1 of its super-band.
All inputs are finite; a program needn't handle non-finite values.
Results may differ from the reference program's by a relative error of at most 0.00005.
Values sent between devices are 32-bit elements; how exact they have to be, the bound alone decides.
A program may use at most 64 MiB of HBM per device.

```python
import math
import jax
import jax.numpy as jnp
from jax import lax

SLOTS = 32
WING = 128
HOP = 2
SPAN = 1024
LPD = 2048
BAND = 65536
BINS = 524288
LINES = 1048576
N_GRP = 8
N_DEV = 64


def draw_line_bin(key, part):
    first, second, third = jax.random.split(jax.random.fold_in(key, 11), 3)
    devices = N_GRP * N_DEV
    owner = jnp.arange(LINES) // LPD
    member = owner % N_DEV
    centre = jax.random.randint(first, (devices,), 0, SPAN)[owner] + member * SPAN
    radius = jax.random.randint(second, (devices,), SPAN // 4, (HOP + 1) * SPAN)[owner]
    raw = jax.random.randint(third, (LINES,), 0, 2 ** 24)
    offset = raw % (2 * radius + 1) - radius
    lowest = jnp.maximum(0, (member - HOP) * SPAN)
    highest = jnp.minimum(BAND, (member + HOP + 1) * SPAN) - 1
    return jnp.clip(centre + offset, lowest, highest).astype(jnp.int32)


def place_ends(values, rng, low, high):
    extent = values.shape
    index_at = [jax.random.randint(jax.random.fold_in(rng, axis), (), 0, extent[axis]) for axis in range(len(extent))]
    values = values.at[tuple(index_at)].set(low)
    longest = extent.index(max(extent))
    index_at[longest] = (index_at[longest] + 1) % extent[longest]
    return values.at[tuple(index_at)].set(high)


def steps_of(rng, extent, shards, low, top_value):
    gain = 1.0
    for axis_at, parts in shards:
        draws = jax.random.uniform(jax.random.fold_in(jax.random.fold_in(rng, 6), axis_at), (parts,), jnp.float32, low / len(shards), top_value / len(shards))
        gain = gain * jnp.repeat(jnp.exp(draws), extent[axis_at] // parts).reshape((-1,) + (1,) * (len(extent) - 1 - axis_at))
    return gain


def setup_inputs(seed: int = 0) -> dict:
    key_list = jax.random.split(jax.random.key(seed), 9)
    return {
        "line_bin": draw_line_bin(jax.random.fold_in(key_list[8], 71), 0),
        "line_slot": place_ends(jax.random.randint(key_list[1], (LINES,), 0, SLOTS), jax.random.fold_in(key_list[1], 1), 0, SLOTS - 1).astype(jnp.int32),
        "strength": jnp.clip(jnp.exp(math.log(1.0) - 2.9957323 * jax.random.uniform(key_list[2], (LINES,), jnp.float32) ** steps_of(key_list[2], (LINES,), ((0, 512),), -0.2, 0.2)), 0.05, 1.0),
        "line_count": place_ends(jax.random.randint(key_list[3], (N_GRP * N_DEV,), LPD // 2, LPD + 1), jax.random.fold_in(key_list[3], 1), LPD // 2, LPD).astype(jnp.int32),
        "gauss_width": jnp.clip(jnp.exp(jax.random.uniform(key_list[4], (SLOTS,), jnp.float32, math.log(2.0), math.log(40.0))), 2.0, 40.0),
        "lorentz_width": jnp.clip(jnp.exp(jax.random.uniform(key_list[5], (SLOTS,), jnp.float32, math.log(1.0), math.log(30.0))), 1.0, 30.0),
        "mixing": jnp.clip(jax.random.uniform(key_list[6], (SLOTS,), jnp.float32, 0.1, 0.9), 0.1, 0.9),
        "profile_factor": jnp.clip(jax.random.uniform(key_list[7], (SLOTS, 2 * WING + 1), jnp.float32, 0.25, 1.75), 0.25, 1.75),
    }


def build_kernel(gauss_width, lorentz_width, mixing, profile_factor):
    offset = jnp.arange(-WING, WING + 1).astype(jnp.float32)
    square = offset[None, :] * offset[None, :]
    lorentz = lorentz_width[:, None] * lorentz_width[:, None] / (square + lorentz_width[:, None] * lorentz_width[:, None])
    gauss = jnp.exp(-square / (2.0 * gauss_width[:, None] * gauss_width[:, None]))
    raw = (mixing[:, None] * lorentz + (1.0 - mixing[:, None]) * gauss) * profile_factor
    return raw / jnp.sum(raw, axis=1, keepdims=True)


def reference(line_bin, line_slot, strength, line_count, gauss_width, lorentz_width, mixing, profile_factor):
    position = jnp.arange(LINES).astype(jnp.int32)
    owner = position // LPD
    group = owner // N_DEV
    live = (position % LPD) < line_count[owner]
    weight = jnp.where(live, strength, jnp.float32(0.0))
    flat = line_slot * BINS + group * BAND + line_bin
    grid = jnp.zeros((SLOTS * BINS,), jnp.float32).at[flat].add(weight).reshape(SLOTS, BINS)
    kernel = build_kernel(gauss_width, lorentz_width, mixing, profile_factor)
    spread = lax.conv_general_dilated(grid[None], kernel[:, None, :], (1,), [(WING, WING)], feature_group_count=SLOTS, precision=lax.Precision.HIGHEST)
    return jnp.sum(spread[0], axis=0)
```

```python
import jax
import jax.numpy as jnp
from jax import lax
from jax.experimental import pallas as pl
from jax.experimental.pallas import tpu as pltpu
from jax.sharding import PartitionSpec as P

SLOTS = 32
WING = 128
HOP = 2
SPAN = 1024
LANES = 128
OFFSETS = (-3, 3, -2, 2, -1, 1)
BF16 = jnp.bfloat16
F32 = jnp.float32
ROWS = (2 * HOP + 1) * SPAN // LANES
PART = 32
QUARTERS = LANES // PART
HALF = SLOTS // 2
TALL = 2 * QUARTERS * ROWS
WIDE = PART * HALF
REACH = 3 * LANES


def split(value):
    high = value.astype(BF16)
    low = (value - high.astype(F32)).astype(BF16)
    return high, low


def column(row):
    i = lax.broadcasted_iota(jnp.int32, (SLOTS, SLOTS), 0)
    j = lax.broadcasted_iota(jnp.int32, (SLOTS, SLOTS), 1)
    spread = jnp.where(i == j, jnp.broadcast_to(row, (SLOTS, SLOTS)), 0.0)
    return jnp.sum(spread, axis=1, keepdims=True)


def voigt_table(gauss_ref, lorentz_ref, mixing_ref, factor_ref, padded):
    padded[...] = jnp.zeros((SLOTS, REACH), F32)
    padded[:, 0 : 2 * WING + 1] = factor_ref[...]
    back = LANES - 1 - lax.broadcasted_iota(jnp.int32, (SLOTS, LANES), 1)
    pieces = [
        jnp.take_along_axis(
            padded[:, c * LANES : (c + 1) * LANES], back, axis=1, mode="promise_in_bounds"
        )
        for c in (2, 1, 0)
    ]
    factor = jnp.concatenate(pieces, axis=1)
    m = lax.broadcasted_iota(jnp.int32, (SLOTS, REACH), 1)
    offset = (REACH - 1 - WING - m).astype(F32)
    square = offset * offset
    gauss_width = column(gauss_ref[...])
    lorentz_width = column(lorentz_ref[...])
    mixing = column(mixing_ref[...])
    wide = lorentz_width * lorentz_width
    lorentz = wide / (square + wide)
    gauss = jnp.exp(-square / (2.0 * gauss_width * gauss_width))
    raw = (mixing * lorentz + (1.0 - mixing) * gauss) * factor
    raw = jnp.where(m >= REACH - 1 - 2 * WING, raw, 0.0)
    return raw / jnp.sum(raw, axis=1, keepdims=True)


def kernel(
    n_grp,
    n_dev,
    bin_ref,
    slot_ref,
    strength_ref,
    count_ref,
    gauss_ref,
    lorentz_ref,
    mixing_ref,
    factor_ref,
    out_ref,
    padded,
    t_high,
    t_low,
    a_ref,
    b_ref,
    tiles,
    inbox,
    send_sem,
    recv_sem,
):
    devices = n_grp * n_dev
    dev = lax.axis_index("dev")
    me = lax.axis_index("grp") * n_dev + dev

    barrier = pltpu.get_barrier_semaphore()
    peers = jnp.int32(0)
    for o in OFFSETS:
        there = jnp.logical_and(me + o >= 0, me + o < devices)
        peers = peers + there.astype(jnp.int32)

        @pl.when(there)
        def _():
            pl.semaphore_signal(
                barrier,
                inc=1,
                device_id=((me + o) // n_dev, (me + o) % n_dev),
                device_id_type=pl.DeviceIdType.MESH,
            )

    table = voigt_table(gauss_ref, lorentz_ref, mixing_ref, factor_ref, padded)
    for r in range(PART):
        high, low = split(pltpu.roll(table, r + 2 * LANES + 1, 1))
        for h in range(2):
            t_high[h * WIDE + r * HALF : h * WIDE + (r + 1) * HALF, :] = high[
                h * HALF : (h + 1) * HALF
            ]
            t_low[h * WIDE + r * HALF : h * WIDE + (r + 1) * HALF, :] = low[
                h * HALF : (h + 1) * HALF
            ]

    lines = bin_ref.shape[0] * LANES
    near = bin_ref[...] - (dev - HOP) * SPAN
    slot = slot_ref[...]
    tall = ((slot // HALF) * QUARTERS + (near // PART) % QUARTERS) * ROWS + near // LANES
    wide = (near % PART) * HALF + slot % HALF
    place = lax.broadcasted_iota(jnp.int32, near.shape, 0) * LANES + lax.broadcasted_iota(
        jnp.int32, near.shape, 1
    )
    weight = jnp.where(place < count_ref[...], strength_ref[...], 0.0)
    weight_high = weight.astype(BF16).astype(F32)
    weight_low = weight - weight_high
    wide = jnp.transpose(wide)
    tall_at = lax.broadcasted_iota(jnp.int32, (TALL, LANES), 0)
    wide_at = lax.broadcasted_iota(jnp.int32, (LANES, WIDE), 1)
    for k in range(lines // LANES):
        cols = slice(k * LANES, (k + 1) * LANES)
        hit = tall_at == tall[k : k + 1, :]
        a_ref[0:TALL, cols] = jnp.where(hit, weight_high[k : k + 1, :], 0.0).astype(BF16)
        a_ref[TALL : 2 * TALL, cols] = jnp.where(hit, weight_low[k : k + 1, :], 0.0).astype(BF16)
        b_ref[cols, :] = jnp.where(wide_at == wide[:, k : k + 1], 1.0, 0.0).astype(BF16)
    both = jnp.dot(a_ref[...], b_ref[...], preferred_element_type=F32)
    grid = both[0:TALL] + both[TALL : 2 * TALL]

    rows = QUARTERS * ROWS
    total = jnp.zeros((rows, REACH), F32)
    for h in range(2):
        high, low = split(grid[h * rows : (h + 1) * rows])
        th = t_high[h * WIDE : (h + 1) * WIDE, :]
        tl = t_low[h * WIDE : (h + 1) * WIDE, :]
        total = total + jnp.dot(high, th, preferred_element_type=F32)
        total = total + jnp.dot(low, th, preferred_element_type=F32)
        total = total + jnp.dot(high, tl, preferred_element_type=F32)
    window = total[0:ROWS]
    for quarter in range(1, QUARTERS):
        window = window + pltpu.roll(
            total[quarter * ROWS : (quarter + 1) * ROWS], quarter * PART, 1
        )
    tiles[...] = jnp.zeros(tiles.shape, F32)
    tiles[7 : 7 + ROWS, :] = window[:, 0:LANES]
    tiles[8 : 8 + ROWS, :] += window[:, LANES : 2 * LANES]
    tiles[9 : 9 + ROWS, :] += window[:, 2 * LANES : 3 * LANES]

    def copy(index, o):
        return pltpu.make_async_remote_copy(
            src_ref=tiles.at[pl.ds((3 + o) * 8, 8), :],
            dst_ref=inbox.at[pl.ds(index * 8, 8), :],
            send_sem=send_sem.at[index],
            recv_sem=recv_sem.at[index],
            device_id=((me + o) // n_dev, (me + o) % n_dev),
            device_id_type=pl.DeviceIdType.MESH,
        )

    pl.semaphore_wait(barrier, peers)
    for index, o in enumerate(OFFSETS):
        there = jnp.logical_and(me + o >= 0, me + o < devices)
        source = jnp.logical_and(me - o >= 0, me - o < devices)

        @pl.when(there)
        def _():
            copy(index, o).start()

        @pl.when(jnp.logical_not(source))
        def _():
            inbox[index * 8 : (index + 1) * 8, :] = jnp.zeros((8, LANES), F32)

    for index, o in enumerate(OFFSETS):
        source = jnp.logical_and(me - o >= 0, me - o < devices)

        @pl.when(source)
        def _():
            copy(index, o).wait_recv()

    total = tiles[24:32, :]
    for index in range(len(OFFSETS)):
        total = total + inbox[index * 8 : (index + 1) * 8, :]
    out_ref[...] = total
    for index, o in enumerate(OFFSETS):
        there = jnp.logical_and(me + o >= 0, me + o < devices)

        @pl.when(there)
        def _():
            copy(index, o).wait_send()


def solution(mesh):
    n_grp, n_dev = mesh.shape["grp"], mesh.shape["dev"]

    def body(
        line_bin, line_slot, strength, line_count, gauss_width, lorentz_width, mixing, factor
    ):
        lines = line_bin.shape[0]

        def call(*refs):
            kernel(n_grp, n_dev, *refs)

        vmem = pl.BlockSpec(memory_space=pltpu.VMEM)
        out = pl.pallas_call(
            call,
            out_shape=jax.ShapeDtypeStruct((SPAN // LANES, LANES), F32),
            in_specs=[vmem] * 8,
            out_specs=vmem,
            scratch_shapes=[
                pltpu.VMEM((SLOTS, REACH), F32),
                pltpu.VMEM((2 * WIDE, REACH), BF16),
                pltpu.VMEM((2 * WIDE, REACH), BF16),
                pltpu.VMEM((2 * TALL, lines), BF16),
                pltpu.VMEM((lines, WIDE), BF16),
                pltpu.VMEM((7 * 8, LANES), F32),
                pltpu.VMEM((6 * 8, LANES), F32),
                pltpu.SemaphoreType.DMA((6,)),
                pltpu.SemaphoreType.DMA((6,)),
            ],
            compiler_params=pltpu.CompilerParams(collective_id=0, has_side_effects=True),
            name="voigt",
        )(
            line_bin.reshape(lines // LANES, LANES),
            line_slot.reshape(lines // LANES, LANES),
            strength.reshape(lines // LANES, LANES),
            line_count.reshape(1, 1),
            gauss_width.reshape(1, SLOTS),
            lorentz_width.reshape(1, SLOTS),
            mixing.reshape(1, SLOTS),
            factor,
        )
        return out.reshape(SPAN)

    split_over = P(("grp", "dev"))
    return jax.shard_map(
        body,
        mesh=mesh,
        in_specs=(split_over,) * 4 + (P(),) * 4,
        out_specs=split_over,
        check_vma=False,
    )
```

```python
import jax
import jax.numpy as jnp
from jax import lax
from jax.experimental import pallas as pl
from jax.experimental.pallas import tpu as pltpu
from jax.sharding import PartitionSpec as P

SLOTS = 32
WING = 128
HOP = 2
SPAN = 1024
LANES = 128
OFFSETS = (3, 2, 1, -3, -2, -1)
BF16 = jnp.bfloat16
F32 = jnp.float32
ROWS = (2 * HOP + 1) * SPAN // LANES
PART = 32
QUARTERS = LANES // PART
HALF = SLOTS // 2
WIDE = PART * HALF
REACH = 3 * LANES
CELLS = QUARTERS * ROWS
CUT = 88


def split(value):
    high = value.astype(BF16)
    low = (value - high.astype(F32)).astype(BF16)
    return high, low


def column(row):
    i = lax.broadcasted_iota(jnp.int32, (SLOTS, SLOTS), 0)
    j = lax.broadcasted_iota(jnp.int32, (SLOTS, SLOTS), 1)
    spread = jnp.where(i == j, jnp.broadcast_to(row, (SLOTS, SLOTS)), 0.0)
    return jnp.sum(spread, axis=1, keepdims=True)


def voigt_table(gauss_ref, lorentz_ref, mixing_ref, factor_ref, padded):
    padded[:, 0 : 2 * WING + 1] = factor_ref[...]
    back = LANES - 1 - lax.broadcasted_iota(jnp.int32, (SLOTS, LANES), 1)
    pieces = [
        jnp.take_along_axis(
            padded[:, c * LANES : (c + 1) * LANES], back, axis=1, mode="promise_in_bounds"
        )
        for c in (2, 1, 0)
    ]
    factor = jnp.concatenate(pieces, axis=1)
    m = lax.broadcasted_iota(jnp.int32, (SLOTS, REACH), 1)
    offset = (REACH - 1 - WING - m).astype(F32)
    square = offset * offset
    gauss_width = column(gauss_ref[...])
    lorentz_width = column(lorentz_ref[...])
    mixing = column(mixing_ref[...])
    wide = lorentz_width * lorentz_width
    lorentz = wide / (square + wide)
    gauss = jnp.exp(-square / (2.0 * gauss_width * gauss_width))
    raw = (mixing * lorentz + (1.0 - mixing) * gauss) * factor
    raw = jnp.where(m >= REACH - 1 - 2 * WING, raw, 0.0)
    return raw / jnp.sum(raw, axis=1, keepdims=True)


def conv(grid, t_high, t_low):
    rows = grid.shape[0] // 2
    total = jnp.zeros((rows, REACH), F32)
    for h in range(2):
        part = grid[h * rows : (h + 1) * rows]
        high = part.astype(BF16).astype(F32)
        both = jnp.concatenate([high, part - high], axis=0).astype(BF16)
        th = t_high[h * WIDE : (h + 1) * WIDE, :]
        tl = t_low[h * WIDE : (h + 1) * WIDE, :]
        twice = jnp.dot(both, th, preferred_element_type=F32)
        total = total + twice[0:rows] + twice[rows : 2 * rows]
        total = total + jnp.dot(high.astype(BF16), tl, preferred_element_type=F32)
    return total


def kernel(
    n_grp,
    n_dev,
    bin_hbm,
    slot_hbm,
    strength_hbm,
    count_hbm,
    gauss_hbm,
    lorentz_hbm,
    mixing_hbm,
    factor_hbm,
    own_ref,
    sum_ref,
    bin_ref,
    slot_ref,
    strength_ref,
    count_ref,
    gauss_ref,
    lorentz_ref,
    mixing_ref,
    factor_ref,
    padded,
    t_high,
    t_low,
    a_ref,
    b_ref,
    stage,
    upper,
    lower,
    inbox,
    in_sem,
    send_sem,
    recv_sem,
):
    devices = n_grp * n_dev
    dev = lax.axis_index("dev")
    me = lax.axis_index("grp") * n_dev + dev

    barrier = pltpu.get_barrier_semaphore()
    peers = jnp.int32(0)
    for o in OFFSETS:
        there = jnp.logical_and(me + o >= 0, me + o < devices)
        peers = peers + there.astype(jnp.int32)

        @pl.when(there)
        def _():
            pl.semaphore_signal(
                barrier,
                inc=1,
                device_id=((me + o) // n_dev, (me + o) % n_dev),
                device_id_type=pl.DeviceIdType.MESH,
            )

    loads = [
        pltpu.make_async_copy(source, target, in_sem.at[i])
        for i, (source, target) in enumerate(
            (
                (bin_hbm, bin_ref),
                (slot_hbm, slot_ref),
                (strength_hbm, strength_ref),
                (count_hbm, count_ref),
                (gauss_hbm, gauss_ref),
                (lorentz_hbm, lorentz_ref),
                (mixing_hbm, mixing_ref),
                (factor_hbm, factor_ref),
            )
        )
    ]
    for load in loads:
        load.start()
    padded[...] = jnp.zeros((SLOTS, REACH), F32)
    for index, o in enumerate(OFFSETS):
        source = jnp.logical_and(me - o >= 0, me - o < devices)

        @pl.when(jnp.logical_not(source))
        def _():
            inbox[index * 8 : (index + 1) * 8, :] = jnp.zeros((8, LANES), F32)

    for load in loads:
        load.wait()

    table = voigt_table(gauss_ref, lorentz_ref, mixing_ref, factor_ref, padded)
    table_high = table.astype(BF16).astype(F32)
    table_low = table - table_high
    for r in range(PART):
        for source, target in ((table_high, t_high), (table_low, t_low)):
            moved = pltpu.roll(source.astype(BF16), r + 2 * LANES + 1, 1)
            for h in range(2):
                target[h * WIDE + r * HALF : h * WIDE + (r + 1) * HALF, :] = moved[
                    h * HALF : (h + 1) * HALF
                ]

    lines = bin_ref.shape[0] * LANES
    near = bin_ref[...] - (dev - HOP) * SPAN
    slot = slot_ref[...]
    q = near // PART
    half = slot // HALF
    first = jnp.where(q >= CUT, half * (CELLS - CUT) + q - CUT, -1)
    second = jnp.where(q < CUT, half * CUT + q, -1)
    wide = (near % PART) * HALF + slot % HALF
    place = lax.broadcasted_iota(jnp.int32, near.shape, 0) * LANES + lax.broadcasted_iota(
        jnp.int32, near.shape, 1
    )
    weight = jnp.where(place < count_ref[...], strength_ref[...], 0.0)
    weight_high = weight.astype(BF16).astype(F32)
    weight_low = weight - weight_high
    wide = jnp.transpose(wide)
    wide_at = lax.broadcasted_iota(jnp.int32, (LANES, WIDE), 1).astype(jnp.int16)
    zero = jnp.zeros((16, LANES), BF16)

    def tile_of(value, k, dtype):
        return jnp.broadcast_to(value[k : k + 1, :], (16, LANES)).astype(dtype)

    def fill_a(place, base, tall):
        for k in range(lines // LANES):
            cols = slice(k * LANES, (k + 1) * LANES)
            at = tile_of(place, k, jnp.int16)
            high = tile_of(weight_high, k, BF16)
            low = tile_of(weight_low, k, BF16)
            for i in range(tall // 16):
                spot = (lax.broadcasted_iota(jnp.int32, (16, LANES), 0) + i * 16).astype(jnp.int16)
                hit = at == spot
                a_ref[base + i * 16 : base + (i + 1) * 16, cols] = jnp.where(hit, high, zero)
                a_ref[base + tall + i * 16 : base + tall + (i + 1) * 16, cols] = jnp.where(
                    hit, low, zero
                )

    def fill_b():
        for k in range(lines // LANES):
            col = jnp.broadcast_to(wide[:, k : k + 1], (LANES, WIDE)).astype(jnp.int16)
            b_ref[k * LANES : (k + 1) * LANES, :] = jnp.where(
                col == wide_at, jnp.ones((LANES, WIDE), BF16), jnp.zeros((LANES, WIDE), BF16)
            )

    def deposit(base, tall):
        both = jnp.dot(a_ref[base : base + 2 * tall, :], b_ref[...], preferred_element_type=F32)
        return both[0:tall] + both[tall : 2 * tall]

    def window(total):
        rows = total.shape[0] // QUARTERS
        for c in range(3):
            stage[c, 0 : total.shape[0], :] = total[:, c * LANES : (c + 1) * LANES]

        def every(quarter):
            return jnp.concatenate(
                [stage[c, pl.ds(quarter, rows, stride=QUARTERS), :] for c in range(3)], axis=1
            )

        value = every(0)
        for quarter in range(1, QUARTERS):
            value = value + pltpu.roll(every(quarter), quarter * PART, 1)
        return value

    def spread(target, at, value):
        rows = value.shape[0]
        target[...] = jnp.zeros(target.shape, F32)
        target[at : at + rows, :] = value[:, 0:LANES]
        target[at + 1 : at + 1 + rows, :] += value[:, LANES : 2 * LANES]
        target[at + 2 : at + 2 + rows, :] += value[:, 2 * LANES : 3 * LANES]

    def copy(index):
        o = OFFSETS[index]
        return pltpu.make_async_remote_copy(
            src_ref=upper.at[pl.ds(o * 8, 8), :] if o > 0 else lower.at[pl.ds((3 + o) * 8, 8), :],
            dst_ref=inbox.at[pl.ds(index * 8, 8), :],
            send_sem=send_sem.at[index],
            recv_sem=recv_sem.at[index],
            device_id=((me + o) // n_dev, (me + o) % n_dev),
            device_id_type=pl.DeviceIdType.MESH,
        )

    def send(index):
        o = OFFSETS[index]

        @pl.when(jnp.logical_and(me + o >= 0, me + o < devices))
        def _():
            copy(index).start()

    fill_b()
    fill_a(first, 0, 2 * (CELLS - CUT))
    far = window(conv(deposit(0, 2 * (CELLS - CUT)), t_high, t_low))
    spread(upper, (CUT // QUARTERS + 7) - 24, far)
    pl.semaphore_wait(barrier, peers)
    for index in range(3):
        send(index)

    base = 4 * (CELLS - CUT)
    fill_a(second, base, 2 * CUT)
    close = window(conv(deposit(base, 2 * CUT), t_high, t_low))
    spread(lower, 7, close)
    for index in range(3, 6):
        send(index)

    own_ref[...] = lower[24:32, :] + upper[0:8, :]
    for index, o in enumerate(OFFSETS):

        @pl.when(jnp.logical_and(me - o >= 0, me - o < devices))
        def _():
            copy(index).wait_recv()

    total = inbox[0:8, :]
    for index in range(1, len(OFFSETS)):
        total = total + inbox[index * 8 : (index + 1) * 8, :]
    sum_ref[...] = total
    for index, o in enumerate(OFFSETS):

        @pl.when(jnp.logical_and(me + o >= 0, me + o < devices))
        def _():
            copy(index).wait_send()


def solution(mesh):
    n_grp, n_dev = mesh.shape["grp"], mesh.shape["dev"]

    def body(
        line_bin, line_slot, strength, line_count, gauss_width, lorentz_width, mixing, factor
    ):
        lines = line_bin.shape[0]

        def call(*refs):
            kernel(n_grp, n_dev, *refs)

        vmem = pl.BlockSpec(memory_space=pltpu.VMEM)
        hbm = pl.BlockSpec(memory_space=pl.ANY)
        piece = jax.ShapeDtypeStruct((SPAN // LANES, LANES), F32)
        own, received = pl.pallas_call(
            call,
            out_shape=(piece, piece),
            in_specs=[hbm] * 8,
            out_specs=(vmem, vmem),
            scratch_shapes=[
                pltpu.VMEM((lines // LANES, LANES), jnp.int32),
                pltpu.VMEM((lines // LANES, LANES), jnp.int32),
                pltpu.VMEM((lines // LANES, LANES), F32),
                pltpu.VMEM((1, 1), jnp.int32),
                pltpu.VMEM((1, SLOTS), F32),
                pltpu.VMEM((1, SLOTS), F32),
                pltpu.VMEM((1, SLOTS), F32),
                pltpu.VMEM((SLOTS, 2 * WING + 1), F32),
                pltpu.VMEM((SLOTS, REACH), F32),
                pltpu.VMEM((2 * WIDE, REACH), BF16),
                pltpu.VMEM((2 * WIDE, REACH), BF16),
                pltpu.VMEM((4 * CELLS, lines), BF16),
                pltpu.VMEM((lines, WIDE), BF16),
                pltpu.VMEM((3, CUT, LANES), F32),
                pltpu.VMEM((4 * 8, LANES), F32),
                pltpu.VMEM((4 * 8, LANES), F32),
                pltpu.VMEM((6 * 8, LANES), F32),
                pltpu.SemaphoreType.DMA((8,)),
                pltpu.SemaphoreType.DMA((6,)),
                pltpu.SemaphoreType.DMA((6,)),
            ],
            compiler_params=pltpu.CompilerParams(collective_id=0, has_side_effects=True),
            name="voigt",
        )(
            line_bin.reshape(lines // LANES, LANES),
            line_slot.reshape(lines // LANES, LANES),
            strength.reshape(lines // LANES, LANES),
            line_count.reshape(1, 1),
            gauss_width.reshape(1, SLOTS),
            lorentz_width.reshape(1, SLOTS),
            mixing.reshape(1, SLOTS),
            factor,
        )
        return (own + received).reshape(SPAN)

    split_over = P(("grp", "dev"))
    return jax.shard_map(
        body,
        mesh=mesh,
        in_specs=(split_over,) * 4 + (P(),) * 4,
        out_specs=split_over,
        check_vma=False,
    )
```

```python
import jax
import jax.numpy as jnp
from jax import lax
from jax.experimental import pallas as pl
from jax.experimental.pallas import tpu as pltpu
from jax.sharding import PartitionSpec as P

SLOTS = 32
WING = 128
HOP = 2
SPAN = 1024
LANES = 128
OFFSETS = (3, 2, 1, -3, -2, -1)
BF16 = jnp.bfloat16
F32 = jnp.float32
ROWS = (2 * HOP + 1) * SPAN // LANES
PART = 16
SUBS = LANES // PART
WIDE = PART * SLOTS
REACH = 3 * LANES
CELLS = SUBS * ROWS
CUT = 176


GRANT = 24 << 20


def split(value):
    high = value.astype(BF16)
    low = (value - high.astype(F32)).astype(BF16)
    return high, low


def column(row):
    i = lax.broadcasted_iota(jnp.int32, (SLOTS, SLOTS), 0)
    j = lax.broadcasted_iota(jnp.int32, (SLOTS, SLOTS), 1)
    spread = jnp.where(i == j, jnp.broadcast_to(row, (SLOTS, SLOTS)), 0.0)
    return jnp.sum(spread, axis=1, keepdims=True)


def voigt_table(gauss_ref, lorentz_ref, mixing_ref, factor_ref, padded):
    padded[:, 0 : 2 * WING + 1] = factor_ref[...]
    back = LANES - 1 - lax.broadcasted_iota(jnp.int32, (SLOTS, LANES), 1)
    pieces = [
        jnp.take_along_axis(
            padded[:, c * LANES : (c + 1) * LANES], back, axis=1, mode="promise_in_bounds"
        )
        for c in (2, 1, 0)
    ]
    factor = jnp.concatenate(pieces, axis=1)
    m = lax.broadcasted_iota(jnp.int32, (SLOTS, REACH), 1)
    offset = (REACH - 1 - WING - m).astype(F32)
    square = offset * offset
    gauss_width = column(gauss_ref[...])
    lorentz_width = column(lorentz_ref[...])
    mixing = column(mixing_ref[...])
    wide = lorentz_width * lorentz_width
    lorentz = wide / (square + wide)
    gauss = jnp.exp(-square / (2.0 * gauss_width * gauss_width))
    raw = (mixing * lorentz + (1.0 - mixing) * gauss) * factor
    raw = jnp.where(m >= REACH - 1 - 2 * WING, raw, 0.0)
    return raw / jnp.sum(raw, axis=1, keepdims=True)


def conv(grid, t_high, t_low):
    rows = grid.shape[0]
    high = grid.astype(BF16).astype(F32)
    both = jnp.concatenate([high, grid - high], axis=0).astype(BF16)
    twice = jnp.dot(both, t_high[...], preferred_element_type=F32)
    rest = jnp.dot(high.astype(BF16), t_low[...], preferred_element_type=F32)
    return twice[0:rows] + twice[rows : 2 * rows] + rest


def kernel(
    n_grp,
    n_dev,
    bin_hbm,
    slot_hbm,
    strength_hbm,
    count_ref,
    gauss_hbm,
    lorentz_hbm,
    mixing_hbm,
    factor_hbm,
    own_ref,
    sum_ref,
    bin_ref,
    slot_ref,
    strength_ref,
    gauss_ref,
    lorentz_ref,
    mixing_ref,
    factor_ref,
    padded,
    t_high,
    t_low,
    a_ref,
    b_ref,
    stage,
    upper,
    lower,
    inbox,
    in_sem,
    send_sem,
    recv_sem,
):
    devices = n_grp * n_dev
    dev = lax.axis_index("dev")
    me = lax.axis_index("grp") * n_dev + dev

    loads = [
        pltpu.make_async_copy(source, target, in_sem.at[i])
        for i, (source, target) in enumerate(
            (
                (bin_hbm, bin_ref),
                (slot_hbm, slot_ref),
                (strength_hbm, strength_ref),
                (gauss_hbm, gauss_ref),
                (lorentz_hbm, lorentz_ref),
                (mixing_hbm, mixing_ref),
                (factor_hbm, factor_ref),
            )
        )
    ]
    for load in loads:
        load.start()
    barrier = pltpu.get_barrier_semaphore()
    peers = jnp.int32(0)
    for o in OFFSETS:
        there = jnp.logical_and(me + o >= 0, me + o < devices)
        peers = peers + there.astype(jnp.int32)

        @pl.when(there)
        def _():
            pl.semaphore_signal(
                barrier,
                inc=1,
                device_id=(lax.div(me + o, n_dev), lax.rem(me + o, n_dev)),
                device_id_type=pl.DeviceIdType.MESH,
            )

    padded[...] = jnp.zeros((SLOTS, REACH), F32)
    for index, o in enumerate(OFFSETS):
        source = jnp.logical_and(me - o >= 0, me - o < devices)

        @pl.when(jnp.logical_not(source))
        def _():
            inbox[index * 8 : (index + 1) * 8, :] = jnp.zeros((8, LANES), F32)

    for load in loads:
        load.wait()

    table = voigt_table(gauss_ref, lorentz_ref, mixing_ref, factor_ref, padded)
    table_high, table_low = split(table)
    for r in range(PART):
        rows = slice(r * SLOTS, (r + 1) * SLOTS)
        t_high[rows, :] = pltpu.roll(table_high, r + 2 * LANES + 1, 1)
        t_low[rows, :] = pltpu.roll(table_low, r + 2 * LANES + 1, 1)

    lines = bin_ref.shape[0] * LANES
    near = bin_ref[...] - (dev - HOP) * SPAN
    slot = slot_ref[...]
    q = near // PART
    first = jnp.where(q >= CUT, q - CUT, -1)
    second = jnp.where(q < CUT, q, -1)
    wide = (near % PART) * SLOTS + slot
    place = lax.broadcasted_iota(jnp.int32, near.shape, 0) * LANES + lax.broadcasted_iota(
        jnp.int32, near.shape, 1
    )
    weight = jnp.where(place < count_ref[0], strength_ref[...], 0.0)
    weight_high = weight.astype(BF16).astype(F32)
    weight_low = weight - weight_high
    wide = jnp.transpose(wide)
    wide_at = lax.broadcasted_iota(jnp.int32, (LANES, WIDE), 1).astype(jnp.int16)
    zero = jnp.zeros((16, LANES), BF16)

    def tile_of(value, k, dtype):
        return jnp.broadcast_to(value[k : k + 1, :], (16, LANES)).astype(dtype)

    def fill_a(place, base, tall):
        for k in range(lines // LANES):
            cols = slice(k * LANES, (k + 1) * LANES)
            at = tile_of(place, k, jnp.int16)
            high = tile_of(weight_high, k, BF16)
            low = tile_of(weight_low, k, BF16)
            for i in range(tall // 16):
                spot = (lax.broadcasted_iota(jnp.int32, (16, LANES), 0) + i * 16).astype(jnp.int16)
                hit = at == spot
                a_ref[base + i * 16 : base + (i + 1) * 16, cols] = jnp.where(hit, high, zero)
                a_ref[base + tall + i * 16 : base + tall + (i + 1) * 16, cols] = jnp.where(
                    hit, low, zero
                )

    def fill_b():
        for k in range(lines // LANES):
            col = jnp.broadcast_to(wide[:, k : k + 1], (LANES, WIDE)).astype(jnp.int16)
            b_ref[k * LANES : (k + 1) * LANES, :] = jnp.where(
                col == wide_at, jnp.ones((LANES, WIDE), BF16), jnp.zeros((LANES, WIDE), BF16)
            )

    def deposit(base, tall):
        both = jnp.dot(a_ref[base : base + 2 * tall, :], b_ref[...], preferred_element_type=F32)
        return both[0:tall] + both[tall : 2 * tall]

    def window(total):
        rows = total.shape[0] // SUBS
        for c in range(3):
            stage[c, 0 : total.shape[0], :] = total[:, c * LANES : (c + 1) * LANES]

        def every(sub):
            return jnp.concatenate(
                [stage[c, pl.ds(sub, rows, stride=SUBS), :] for c in range(3)], axis=1
            )

        value = every(0)
        for sub in range(1, SUBS):
            value = value + pltpu.roll(every(sub), sub * PART, 1)
        return value

    def spread(target, at, value):
        rows = value.shape[0]
        target[...] = jnp.zeros(target.shape, F32)
        target[at : at + rows, :] = value[:, 0:LANES]
        target[at + 1 : at + 1 + rows, :] += value[:, LANES : 2 * LANES]
        target[at + 2 : at + 2 + rows, :] += value[:, 2 * LANES : 3 * LANES]

    def copy(index):
        o = OFFSETS[index]
        return pltpu.make_async_remote_copy(
            src_ref=upper.at[pl.ds(o * 8, 8), :] if o > 0 else lower.at[pl.ds((3 + o) * 8, 8), :],
            dst_ref=inbox.at[pl.ds(index * 8, 8), :],
            send_sem=send_sem.at[index],
            recv_sem=recv_sem.at[index],
            device_id=(lax.div(me + o, n_dev), lax.rem(me + o, n_dev)),
            device_id_type=pl.DeviceIdType.MESH,
        )

    def send(index):
        o = OFFSETS[index]

        @pl.when(jnp.logical_and(me + o >= 0, me + o < devices))
        def _():
            copy(index).start()

    fill_b()
    fill_a(first, 0, CELLS - CUT)
    far = window(conv(deposit(0, CELLS - CUT), t_high, t_low))
    spread(upper, (CUT // SUBS + 7) - 24, far)
    pl.semaphore_wait(barrier, peers)
    for index in range(3):
        send(index)

    base = 2 * (CELLS - CUT)
    fill_a(second, base, CUT)
    close = window(conv(deposit(base, CUT), t_high, t_low))
    spread(lower, 7, close)
    for index in range(3, 6):
        send(index)

    own_ref[...] = lower[24:32, :] + upper[0:8, :]
    for index, o in enumerate(OFFSETS):

        @pl.when(jnp.logical_and(me - o >= 0, me - o < devices))
        def _():
            copy(index).wait_recv()

    total = inbox[0:8, :]
    for index in range(1, len(OFFSETS)):
        total = total + inbox[index * 8 : (index + 1) * 8, :]
    sum_ref[...] = total
    for index, o in enumerate(OFFSETS):

        @pl.when(jnp.logical_and(me + o >= 0, me + o < devices))
        def _():
            copy(index).wait_send()


def solution(mesh):
    n_grp, n_dev = mesh.shape["grp"], mesh.shape["dev"]

    def body(
        line_bin, line_slot, strength, line_count, gauss_width, lorentz_width, mixing, factor
    ):
        lines = line_bin.shape[0]

        def call(*refs):
            kernel(n_grp, n_dev, *refs)

        vmem = pl.BlockSpec(memory_space=pltpu.VMEM)
        hbm = pl.BlockSpec(memory_space=pltpu.HBM)
        piece = jax.ShapeDtypeStruct((SPAN // LANES, LANES), F32)
        own, received = pl.pallas_call(
            call,
            out_shape=(piece, piece),
            in_specs=[hbm] * 3 + [pl.BlockSpec(memory_space=pltpu.SMEM)] + [hbm] * 4,
            out_specs=(vmem, vmem),
            scratch_shapes=[
                pltpu.VMEM((lines // LANES, LANES), jnp.int32),
                pltpu.VMEM((lines // LANES, LANES), jnp.int32),
                pltpu.VMEM((lines // LANES, LANES), F32),
                pltpu.VMEM((1, SLOTS), F32),
                pltpu.VMEM((1, SLOTS), F32),
                pltpu.VMEM((1, SLOTS), F32),
                pltpu.VMEM((SLOTS, 2 * WING + 1), F32),
                pltpu.VMEM((SLOTS, REACH), F32),
                pltpu.VMEM((WIDE, REACH), BF16),
                pltpu.VMEM((WIDE, REACH), BF16),
                pltpu.VMEM((2 * CELLS, lines), BF16),
                pltpu.VMEM((lines, WIDE), BF16),
                pltpu.VMEM((3, CUT, LANES), F32),
                pltpu.VMEM((4 * 8, LANES), F32),
                pltpu.VMEM((4 * 8, LANES), F32),
                pltpu.VMEM((6 * 8, LANES), F32),
                pltpu.SemaphoreType.DMA((7,)),
                pltpu.SemaphoreType.DMA((6,)),
                pltpu.SemaphoreType.DMA((6,)),
            ],
            compiler_params=pltpu.CompilerParams(
                collective_id=0, has_side_effects=True, vmem_limit_bytes=GRANT
            ),
            name="voigt",
        )(
            *(
                value if value.size == 1 else pltpu.with_memory_space_constraint(value, pltpu.HBM)
                for value in (
                    line_bin.reshape(lines // LANES, LANES),
                    line_slot.reshape(lines // LANES, LANES),
                    strength.reshape(lines // LANES, LANES),
                    line_count,
                    gauss_width.reshape(1, SLOTS),
                    lorentz_width.reshape(1, SLOTS),
                    mixing.reshape(1, SLOTS),
                    factor,
                )
            )
        )
        return (own + received).reshape(SPAN)

    split_over = P(("grp", "dev"))
    return jax.shard_map(
        body,
        mesh=mesh,
        in_specs=(split_over,) * 4 + (P(),) * 4,
        out_specs=split_over,
        check_vma=False,
    )
```

```python
import jax
import jax.numpy as jnp
from jax import lax
from jax.experimental import pallas as pl
from jax.experimental.pallas import tpu as pltpu
from jax.sharding import PartitionSpec as P

SLOTS = 32
WING = 128
HOP = 2
SPAN = 1024
LANES = 128
OFFSETS = (3, 2, 1, -3, -2, -1)
BF16 = jnp.bfloat16
F32 = jnp.float32
ROWS = (2 * HOP + 1) * SPAN // LANES
PART = 16
SUBS = LANES // PART
WIDE = PART * SLOTS
REACH = 3 * LANES
CELLS = SUBS * ROWS
MID = 184


GRANT = 24 << 20


def split(value):
    high = value.astype(BF16)
    low = (value - high.astype(F32)).astype(BF16)
    return high, low


def column(row):
    i = lax.broadcasted_iota(jnp.int32, (SLOTS, SLOTS), 0)
    j = lax.broadcasted_iota(jnp.int32, (SLOTS, SLOTS), 1)
    spread = jnp.where(i == j, jnp.broadcast_to(row, (SLOTS, SLOTS)), 0.0)
    return jnp.sum(spread, axis=1, keepdims=True)


def voigt_table(gauss_ref, lorentz_ref, mixing_ref, factor_ref, padded):
    padded[:, 0 : 2 * WING + 1] = factor_ref[...]
    back = LANES - 1 - lax.broadcasted_iota(jnp.int32, (SLOTS, LANES), 1)
    pieces = [
        jnp.take_along_axis(
            padded[:, c * LANES : (c + 1) * LANES], back, axis=1, mode="promise_in_bounds"
        )
        for c in (2, 1, 0)
    ]
    factor = jnp.concatenate(pieces, axis=1)
    m = lax.broadcasted_iota(jnp.int32, (SLOTS, REACH), 1)
    offset = (REACH - 1 - WING - m).astype(F32)
    square = offset * offset
    gauss_width = column(gauss_ref[...])
    lorentz_width = column(lorentz_ref[...])
    mixing = column(mixing_ref[...])
    wide = lorentz_width * lorentz_width
    lorentz = wide / (square + wide)
    gauss = jnp.exp(-square / (2.0 * gauss_width * gauss_width))
    raw = (mixing * lorentz + (1.0 - mixing) * gauss) * factor
    raw = jnp.where(m >= REACH - 1 - 2 * WING, raw, 0.0)
    return raw / jnp.sum(raw, axis=1, keepdims=True)


def conv(grid, t_high, t_low):
    rows = grid.shape[0]
    high = grid.astype(BF16).astype(F32)
    both = jnp.concatenate([high, grid - high], axis=0).astype(BF16)
    twice = jnp.dot(both, t_high[...], preferred_element_type=F32)
    rest = jnp.dot(high.astype(BF16), t_low[...], preferred_element_type=F32)
    return twice[0:rows] + twice[rows : 2 * rows] + rest


def kernel(
    n_grp,
    n_dev,
    bin_hbm,
    slot_hbm,
    strength_hbm,
    count_ref,
    gauss_hbm,
    lorentz_hbm,
    mixing_hbm,
    factor_hbm,
    own_ref,
    sum_ref,
    bin_ref,
    slot_ref,
    strength_ref,
    gauss_ref,
    lorentz_ref,
    mixing_ref,
    factor_ref,
    padded,
    t_high,
    t_low,
    stage,
    upper,
    lower,
    inbox,
    in_sem,
    send_sem,
    recv_sem,
    ready_sem,
):
    devices = n_grp * n_dev
    dev = lax.axis_index("dev")
    me = lax.axis_index("grp") * n_dev + dev

    loads = [
        pltpu.make_async_copy(source, target, in_sem.at[i])
        for i, (source, target) in enumerate(
            (
                (bin_hbm, bin_ref),
                (slot_hbm, slot_ref),
                (strength_hbm, strength_ref),
                (gauss_hbm, gauss_ref),
                (lorentz_hbm, lorentz_ref),
                (mixing_hbm, mixing_ref),
                (factor_hbm, factor_ref),
            )
        )
    ]
    for load in loads:
        load.start()
    def exists(o):
        return me + o < devices if o > 0 else me + o >= 0

    def tell(semaphore, o):
        @pl.when(exists(o))
        def _():
            pl.semaphore_signal(
                semaphore,
                inc=1,
                device_id=(lax.div(me + o, n_dev), lax.rem(me + o, n_dev)),
                device_id_type=pl.DeviceIdType.MESH,
            )

    barrier = pltpu.get_barrier_semaphore()
    above = jnp.int32(0)
    for o in (1, 2, 3):
        above = above + exists(o).astype(jnp.int32)
        tell(barrier, -o)
    padded[...] = jnp.zeros((SLOTS, REACH), F32)
    for index, o in enumerate(OFFSETS):
        @pl.when(jnp.logical_not(exists(-o)))
        def _():
            inbox[index * 8 : (index + 1) * 8, :] = jnp.zeros((8, LANES), F32)

    for load in loads:
        load.wait()

    table = voigt_table(gauss_ref, lorentz_ref, mixing_ref, factor_ref, padded)
    table_high, table_low = split(table)
    for r in range(PART):
        rows = slice(r * SLOTS, (r + 1) * SLOTS)
        t_high[rows, :] = pltpu.roll(table_high, r + 2 * LANES + 1, 1)
        t_low[rows, :] = pltpu.roll(table_low, r + 2 * LANES + 1, 1)

    lines = bin_ref.shape[0] * LANES
    near = bin_ref[...] - (dev - HOP) * SPAN
    slot = slot_ref[...]
    q = near // PART
    wide = (near % PART) * SLOTS + slot
    place = lax.broadcasted_iota(jnp.int32, near.shape, 0) * LANES + lax.broadcasted_iota(
        jnp.int32, near.shape, 1
    )
    weight = jnp.where(place < count_ref[0], strength_ref[...], 0.0)
    weight_high = weight.astype(BF16).astype(F32)
    weight_low = weight - weight_high
    wide = jnp.transpose(wide)
    lane = lax.broadcasted_iota(jnp.int32, (LANES, LANES), 1)
    spot = lax.broadcasted_iota(jnp.int32, (16, LANES), 0)
    blocks = lines // LANES
    zero = jnp.zeros((16, LANES), BF16)

    def tile_of(value, k, dtype):
        return jnp.broadcast_to(value[k : k + 1, :], (16, LANES)).astype(dtype)

    def column_of(k):
        return jnp.broadcast_to(wide[:, k : k + 1], (LANES, LANES)).astype(jnp.int16)

    def one_hot():
        rows = []
        for k in range(blocks):
            at = column_of(k)
            rows.append(
                jnp.concatenate(
                    [
                        jnp.where(
                            at == (lane + c * LANES).astype(jnp.int16),
                            jnp.ones((LANES, LANES), BF16),
                            jnp.zeros((LANES, LANES), BF16),
                        )
                        for c in range(WIDE // LANES)
                    ],
                    axis=1,
                )
            )
        return jnp.concatenate(rows, axis=0)

    def weighted(low_cell, high_cell):
        rows = high_cell - low_cell
        inside = jnp.logical_and(q >= low_cell, q < high_cell)
        place = jnp.where(inside, q - low_cell, -4 * CELLS)
        cols = []
        for k in range(blocks):
            at = tile_of(place, k, jnp.int16)
            at_low = tile_of(place + rows, k, jnp.int16)
            high = tile_of(weight_high, k, BF16)
            low = tile_of(weight_low, k, BF16)
            tiles = []
            for i in range(2 * rows // 16):
                here = (spot + i * 16).astype(jnp.int16)
                value = zero
                if (i + 1) * 16 > rows:
                    value = jnp.where(at_low == here, low, value)
                if i * 16 < rows:
                    value = jnp.where(at == here, high, value)
                tiles.append(value)
            cols.append(jnp.concatenate(tiles, axis=0))
        return jnp.concatenate(cols, axis=1)

    def deposit(low_cell, high_cell):
        rows = high_cell - low_cell
        both = jnp.dot(
            weighted(low_cell, high_cell), one_hot(), preferred_element_type=F32
        )
        return both[0:rows] + both[rows : 2 * rows]

    def window(total):
        rows = total.shape[0] // SUBS
        for c in range(3):
            stage[c, 0 : total.shape[0], :] = total[:, c * LANES : (c + 1) * LANES]

        def every(sub):
            return jnp.concatenate(
                [stage[c, pl.ds(sub, rows, stride=SUBS), :] for c in range(3)], axis=1
            )

        value = every(0)
        for sub in range(1, SUBS):
            value = value + pltpu.roll(every(sub), sub * PART, 1)
        return value

    def spread(target, at, value):
        rows = value.shape[0]
        target[...] = jnp.zeros(target.shape, F32)
        target[at : at + rows, :] = value[:, 0:LANES]
        target[at + 1 : at + 1 + rows, :] += value[:, LANES : 2 * LANES]
        target[at + 2 : at + 2 + rows, :] += value[:, 2 * LANES : 3 * LANES]

    pieces = tuple(upper.at[pl.ds(i * 8, 8), :] for i in (3, 2, 1)) + tuple(
        lower.at[pl.ds(i * 8, 8), :] for i in range(3)
    )

    def copy(index):
        o = OFFSETS[index]
        return pltpu.make_async_remote_copy(
            src_ref=pieces[index],
            dst_ref=inbox.at[pl.ds(index * 8, 8), :],
            send_sem=send_sem.at[index],
            recv_sem=recv_sem.at[index],
            device_id=(lax.div(me + o, n_dev), lax.rem(me + o, n_dev)),
            device_id_type=pl.DeviceIdType.MESH,
        )

    def send(index):
        @pl.when(exists(OFFSETS[index]))
        def _():
            copy(index).start()

    spread(upper, 6, window(conv(deposit(MID, CELLS), t_high, t_low)))
    @pl.when(exists(1))
    def _():
        pl.semaphore_wait(barrier, above)

    for index in range(3):
        send(index)
    for o in (1, 2, 3):
        tell(ready_sem.at[o - 1], o)

    spread(lower, 7, window(conv(deposit(0, MID), t_high, t_low)))
    own_ref[...] = lower[24:32, :] + upper[0:8, :]
    for index in range(3, 6):
        o = OFFSETS[index]

        @pl.when(exists(o))
        def _():
            pl.semaphore_wait(ready_sem.at[-o - 1], 1)
            copy(index).start()

    for index, o in enumerate(OFFSETS):

        @pl.when(exists(-o))
        def _():
            copy(index).wait_recv()

    total = inbox[0:8, :]
    for index in range(1, len(OFFSETS)):
        total = total + inbox[index * 8 : (index + 1) * 8, :]
    sum_ref[...] = total
    for index, o in enumerate(OFFSETS):

        @pl.when(exists(o))
        def _():
            copy(index).wait_send()


def solution(mesh):
    n_grp, n_dev = mesh.shape["grp"], mesh.shape["dev"]

    def body(
        line_bin, line_slot, strength, line_count, gauss_width, lorentz_width, mixing, factor
    ):
        lines = line_bin.shape[0]

        def call(*refs):
            kernel(n_grp, n_dev, *refs)

        vmem = pl.BlockSpec(memory_space=pltpu.VMEM)
        hbm = pl.BlockSpec(memory_space=pltpu.HBM)
        piece = jax.ShapeDtypeStruct((SPAN // LANES, LANES), F32)
        own, received = pl.pallas_call(
            call,
            out_shape=(piece, piece),
            in_specs=[hbm] * 3 + [pl.BlockSpec(memory_space=pltpu.SMEM)] + [hbm] * 4,
            out_specs=(vmem, vmem),
            scratch_shapes=[
                pltpu.VMEM((lines // LANES, LANES), jnp.int32),
                pltpu.VMEM((lines // LANES, LANES), jnp.int32),
                pltpu.VMEM((lines // LANES, LANES), F32),
                pltpu.VMEM((1, SLOTS), F32),
                pltpu.VMEM((1, SLOTS), F32),
                pltpu.VMEM((1, SLOTS), F32),
                pltpu.VMEM((SLOTS, 2 * WING + 1), F32),
                pltpu.VMEM((SLOTS, REACH), F32),
                pltpu.VMEM((WIDE, REACH), BF16),
                pltpu.VMEM((WIDE, REACH), BF16),
                pltpu.VMEM((3, MID, LANES), F32),
                pltpu.VMEM((4 * 8, LANES), F32),
                pltpu.VMEM((4 * 8, LANES), F32),
                pltpu.VMEM((6 * 8, LANES), F32),
                pltpu.SemaphoreType.DMA((7,)),
                pltpu.SemaphoreType.DMA((6,)),
                pltpu.SemaphoreType.DMA((6,)),
                pltpu.SemaphoreType.REGULAR((3,)),
            ],
            compiler_params=pltpu.CompilerParams(
                collective_id=0, has_side_effects=True, vmem_limit_bytes=GRANT
            ),
            name="voigt",
        )(
            *(
                value if value.size == 1 else pltpu.with_memory_space_constraint(value, pltpu.HBM)
                for value in (
                    line_bin.reshape(lines // LANES, LANES),
                    line_slot.reshape(lines // LANES, LANES),
                    strength.reshape(lines // LANES, LANES),
                    line_count,
                    gauss_width.reshape(1, SLOTS),
                    lorentz_width.reshape(1, SLOTS),
                    mixing.reshape(1, SLOTS),
                    factor,
                )
            )
        )
        return (own + received).reshape(SPAN)

    split_over = P(("grp", "dev"))
    return jax.shard_map(
        body,
        mesh=mesh,
        in_specs=(split_over,) * 4 + (P(),) * 4,
        out_specs=split_over,
        check_vma=False,
    )
```

```python
import jax
import jax.numpy as jnp
from jax import lax
from jax.experimental import pallas as pl
from jax.experimental.pallas import tpu as pltpu
from jax.sharding import PartitionSpec as P

SLOTS = 32
WING = 128
HOP = 2
SPAN = 1024
LANES = 128
ROW = 16
OFFSETS = (3, 2, 1, -2, -1)
SPOTS = ((0, 8), (8, 8), (16, 8), (24, 16), (40, 8))
BF16 = jnp.bfloat16
F32 = jnp.float32
ROWS = (2 * HOP + 1) * SPAN // LANES
PART = 16
SUBS = LANES // PART
WIDE = PART * SLOTS
REACH = 3 * LANES
CELLS = SUBS * ROWS
FAR = 248
MID = 184


GRANT = 24 << 20


def split(value):
    high = value.astype(BF16)
    low = (value - high.astype(F32)).astype(BF16)
    return high, low


def column(row):
    i = lax.broadcasted_iota(jnp.int32, (SLOTS, SLOTS), 0)
    j = lax.broadcasted_iota(jnp.int32, (SLOTS, SLOTS), 1)
    spread = jnp.where(i == j, jnp.broadcast_to(row, (SLOTS, SLOTS)), 0.0)
    return jnp.sum(spread, axis=1, keepdims=True)


def voigt_table(gauss_ref, lorentz_ref, mixing_ref, factor_ref, padded):
    padded[:, 0 : 2 * WING + 1] = factor_ref[...]
    back = LANES - 1 - lax.broadcasted_iota(jnp.int32, (SLOTS, LANES), 1)
    pieces = [
        jnp.take_along_axis(
            padded[:, c * LANES : (c + 1) * LANES], back, axis=1, mode="promise_in_bounds"
        )
        for c in (2, 1, 0)
    ]
    factor = jnp.concatenate(pieces, axis=1)
    m = lax.broadcasted_iota(jnp.int32, (SLOTS, REACH), 1)
    offset = (REACH - 1 - WING - m).astype(F32)
    square = offset * offset
    gauss_width = column(gauss_ref[...])
    lorentz_width = column(lorentz_ref[...])
    mixing = column(mixing_ref[...])
    wide = lorentz_width * lorentz_width
    lorentz = wide / (square + wide)
    gauss = jnp.exp(-square / (2.0 * gauss_width * gauss_width))
    raw = (mixing * lorentz + (1.0 - mixing) * gauss) * factor
    raw = jnp.where(m >= REACH - 1 - 2 * WING, raw, 0.0)
    return raw / jnp.sum(raw, axis=1, keepdims=True)


def conv(grid, t_high, t_low):
    rows = grid.shape[0]
    high = grid.astype(BF16).astype(F32)
    both = jnp.concatenate([high, grid - high], axis=0).astype(BF16)
    twice = jnp.dot(both, t_high[...], preferred_element_type=F32)
    rest = jnp.dot(high.astype(BF16), t_low[...], preferred_element_type=F32)
    return twice[0:rows] + twice[rows : 2 * rows] + rest


def kernel(
    n_grp,
    n_dev,
    bin_hbm,
    slot_hbm,
    strength_hbm,
    count_ref,
    gauss_hbm,
    lorentz_hbm,
    mixing_hbm,
    factor_hbm,
    own_ref,
    sum_ref,
    bin_ref,
    slot_ref,
    strength_ref,
    gauss_ref,
    lorentz_ref,
    mixing_ref,
    factor_ref,
    padded,
    t_high,
    t_low,
    wide_ref,
    stage,
    far,
    middle,
    near_up,
    near_down,
    lower,
    inbox,
    in_sem,
    send_sem,
    recv_sem,
):
    devices = n_grp * n_dev
    dev = lax.axis_index("dev")
    me = lax.axis_index("grp") * n_dev + dev

    loads = [
        pltpu.make_async_copy(source, target, in_sem.at[i])
        for i, (source, target) in enumerate(
            (
                (bin_hbm, bin_ref),
                (slot_hbm, slot_ref),
                (strength_hbm, strength_ref),
                (gauss_hbm, gauss_ref),
                (lorentz_hbm, lorentz_ref),
                (mixing_hbm, mixing_ref),
                (factor_hbm, factor_ref),
            )
        )
    ]
    for load in loads:
        load.start()
    late = lax.rem(dev, ROW) >= ROW // 2

    def exists(o):
        return me + o < devices if o > 0 else me + o >= 0

    def tell(semaphore, o):
        @pl.when(exists(o))
        def _():
            pl.semaphore_signal(
                semaphore,
                inc=1,
                device_id=(lax.div(me + o, n_dev), lax.rem(me + o, n_dev)),
                device_id_type=pl.DeviceIdType.MESH,
            )

    barrier = pltpu.get_barrier_semaphore()
    heard = jnp.int32(0)
    for o in OFFSETS:
        heard = heard + exists(o).astype(jnp.int32)
        tell(barrier, -o)

    padded[...] = jnp.zeros((SLOTS, REACH), F32)
    for index, o in enumerate(OFFSETS):
        @pl.when(jnp.logical_not(exists(-o)))
        def _():
            at, rows = SPOTS[index]
            inbox[at : at + rows, :] = jnp.zeros((rows, LANES), F32)

    for load in loads:
        load.wait()

    table = voigt_table(gauss_ref, lorentz_ref, mixing_ref, factor_ref, padded)
    table_high, table_low = split(table)
    for r in range(PART):
        rows = slice(r * SLOTS, (r + 1) * SLOTS)
        t_high[rows, :] = pltpu.roll(table_high, r + 2 * LANES + 1, 1)
        t_low[rows, :] = pltpu.roll(table_low, r + 2 * LANES + 1, 1)

    lines = bin_ref.shape[0] * LANES
    near = bin_ref[...] - (dev - HOP) * SPAN
    slot = slot_ref[...]
    q = near // PART
    wide = (near % PART) * SLOTS + slot
    place = lax.broadcasted_iota(jnp.int32, near.shape, 0) * LANES + lax.broadcasted_iota(
        jnp.int32, near.shape, 1
    )
    weight = jnp.where(place < count_ref[0], strength_ref[...], 0.0)
    weight_high = weight.astype(BF16).astype(F32)
    weight_low = weight - weight_high
    wide = jnp.transpose(wide)
    lane = lax.broadcasted_iota(jnp.int32, (LANES, LANES), 1)
    spot = lax.broadcasted_iota(jnp.int32, (16, LANES), 0)
    blocks = lines // LANES
    zero = jnp.zeros((16, LANES), BF16)

    def tile_of(value, k, dtype):
        return jnp.broadcast_to(value[k : k + 1, :], (16, LANES)).astype(dtype)

    wide_ref[...] = wide

    def columns(k):
        return jnp.broadcast_to(wide[:, k : k + 1], (LANES, LANES)).astype(jnp.int16)

    def kept(k):
        return jnp.broadcast_to(wide_ref[:, k : k + 1], (LANES, LANES)).astype(jnp.int16)

    def one_hot(column_of):
        rows = []
        for k in range(blocks):
            at = column_of(k)
            rows.append(
                jnp.concatenate(
                    [
                        jnp.where(
                            at == (lane + c * LANES).astype(jnp.int16),
                            jnp.ones((LANES, LANES), BF16),
                            jnp.zeros((LANES, LANES), BF16),
                        )
                        for c in range(WIDE // LANES)
                    ],
                    axis=1,
                )
            )
        return jnp.concatenate(rows, axis=0)

    def weighted(low_cell, high_cell):
        rows = high_cell - low_cell
        inside = jnp.logical_and(q >= low_cell, q < high_cell)
        place = jnp.where(inside, q - low_cell, -4 * CELLS)
        cols = []
        for k in range(blocks):
            at = tile_of(place, k, jnp.int16)
            at_low = tile_of(place + rows, k, jnp.int16)
            high = tile_of(weight_high, k, BF16)
            low = tile_of(weight_low, k, BF16)
            tiles = []
            for i in range(2 * rows // 16):
                here = (spot + i * 16).astype(jnp.int16)
                value = zero
                if (i + 1) * 16 > rows:
                    value = jnp.where(at_low == here, low, value)
                if i * 16 < rows:
                    value = jnp.where(at == here, high, value)
                tiles.append(value)
            cols.append(jnp.concatenate(tiles, axis=0))
        return jnp.concatenate(cols, axis=1)

    def deposit(low_cell, high_cell, column_of):
        rows = high_cell - low_cell
        both = jnp.dot(
            weighted(low_cell, high_cell), one_hot(column_of), preferred_element_type=F32
        )
        return both[0:rows] + both[rows : 2 * rows]

    def window(total):
        rows = total.shape[0] // SUBS
        for c in range(3):
            stage[c, 0 : total.shape[0], :] = total[:, c * LANES : (c + 1) * LANES]

        def every(sub):
            return jnp.concatenate(
                [stage[c, pl.ds(sub, rows, stride=SUBS), :] for c in range(3)], axis=1
            )

        value = every(0)
        for sub in range(1, SUBS):
            value = value + pltpu.roll(every(sub), sub * PART, 1)
        return value

    def spread(target, at, value):
        rows = value.shape[0]
        target[...] = jnp.zeros(target.shape, F32)
        target[at : at + rows, :] = value[:, 0:LANES]
        target[at + 1 : at + 1 + rows, :] += value[:, LANES : 2 * LANES]
        target[at + 2 : at + 2 + rows, :] += value[:, 2 * LANES : 3 * LANES]

    pieces = (far.at[pl.ds(16, 8), :], far.at[pl.ds(8, 8), :], near_up)
    pieces += (lower.at[pl.ds(0, 16), :], near_down)

    def copy(index):
        o = OFFSETS[index]
        return pltpu.make_async_remote_copy(
            src_ref=pieces[index],
            dst_ref=inbox.at[pl.ds(*SPOTS[index]), :],
            send_sem=send_sem.at[index],
            recv_sem=recv_sem.at[index],
            device_id=(lax.div(me + o, n_dev), lax.rem(me + o, n_dev)),
            device_id_type=pl.DeviceIdType.MESH,
        )

    def send(index, condition):
        @pl.when(jnp.logical_and(exists(OFFSETS[index]), condition))
        def _():
            copy(index).start()

    spread(far, 6, window(conv(deposit(FAR, CELLS, columns), t_high, t_low)))

    @pl.when(late)
    def _():
        pl.semaphore_wait(barrier, heard)

    send(0, late)
    send(1, late)

    spread(middle, 6, window(conv(deposit(MID, FAR, kept), t_high, t_low)))
    near_up[...] = middle[8:16, :] + far[0:8, :]
    send(2, late)

    spread(lower, 7, window(conv(deposit(0, MID, kept), t_high, t_low)))
    own_ref[...] = lower[24:32, :] + middle[0:8, :]
    def take(index):
        @pl.when(exists(-OFFSETS[index]))
        def _():
            copy(index).wait_recv()


    @pl.when(jnp.logical_not(late))
    def _():
        pl.semaphore_wait(barrier, heard)

    for index in range(3):
        send(index, jnp.logical_not(late))
    send(3, True)
    take(3)
    near_down[...] = lower[16:24, :] + inbox[24:32, :]
    send(4, True)
    for index in (4, 2, 1, 0):
        take(index)

    total = inbox[0:8, :]
    for at in (8, 16, 32, 40):
        total = total + inbox[at : at + 8, :]
    sum_ref[...] = total
    for index, o in enumerate(OFFSETS):

        @pl.when(exists(o))
        def _():
            copy(index).wait_send()


def solution(mesh):
    n_grp, n_dev = mesh.shape["grp"], mesh.shape["dev"]

    def body(
        line_bin, line_slot, strength, line_count, gauss_width, lorentz_width, mixing, factor
    ):
        lines = line_bin.shape[0]

        def call(*refs):
            kernel(n_grp, n_dev, *refs)

        vmem = pl.BlockSpec(memory_space=pltpu.VMEM)
        hbm = pl.BlockSpec(memory_space=pltpu.HBM)
        piece = jax.ShapeDtypeStruct((SPAN // LANES, LANES), F32)
        own, received = pl.pallas_call(
            call,
            out_shape=(piece, piece),
            in_specs=[hbm] * 3 + [pl.BlockSpec(memory_space=pltpu.SMEM)] + [hbm] * 4,
            out_specs=(vmem, vmem),
            scratch_shapes=[
                pltpu.VMEM((lines // LANES, LANES), jnp.int32),
                pltpu.VMEM((lines // LANES, LANES), jnp.int32),
                pltpu.VMEM((lines // LANES, LANES), F32),
                pltpu.VMEM((1, SLOTS), F32),
                pltpu.VMEM((1, SLOTS), F32),
                pltpu.VMEM((1, SLOTS), F32),
                pltpu.VMEM((SLOTS, 2 * WING + 1), F32),
                pltpu.VMEM((SLOTS, REACH), F32),
                pltpu.VMEM((WIDE, REACH), BF16),
                pltpu.VMEM((WIDE, REACH), BF16),
                pltpu.VMEM((LANES, lines // LANES), jnp.int32),
                pltpu.VMEM((3, MID, LANES), F32),
                pltpu.VMEM((3 * 8, LANES), F32),
                pltpu.VMEM((2 * 8, LANES), F32),
                pltpu.VMEM((8, LANES), F32),
                pltpu.VMEM((8, LANES), F32),
                pltpu.VMEM((4 * 8, LANES), F32),
                pltpu.VMEM((6 * 8, LANES), F32),
                pltpu.SemaphoreType.DMA((7,)),
                pltpu.SemaphoreType.DMA((5,)),
                pltpu.SemaphoreType.DMA((5,)),
            ],
            compiler_params=pltpu.CompilerParams(
                collective_id=0, has_side_effects=True, vmem_limit_bytes=GRANT
            ),
            name="voigt",
        )(
            *(
                value if value.size == 1 else pltpu.with_memory_space_constraint(value, pltpu.HBM)
                for value in (
                    line_bin.reshape(lines // LANES, LANES),
                    line_slot.reshape(lines // LANES, LANES),
                    strength.reshape(lines // LANES, LANES),
                    line_count,
                    gauss_width.reshape(1, SLOTS),
                    lorentz_width.reshape(1, SLOTS),
                    mixing.reshape(1, SLOTS),
                    factor,
                )
            )
        )
        return (own + received).reshape(SPAN)

    split_over = P(("grp", "dev"))
    return jax.shard_map(
        body,
        mesh=mesh,
        in_specs=(split_over,) * 4 + (P(),) * 4,
        out_specs=split_over,
        check_vma=False,
    )
```

```python
import jax
import jax.numpy as jnp
from jax import lax
from jax.experimental import pallas as pl
from jax.experimental.pallas import tpu as pltpu
from jax.sharding import PartitionSpec as P

SLOTS = 32
WING = 128
HOP = 2
SPAN = 1024
LANES = 128
ROW = 16
OFFSETS = (3, 2, 1, -2, -1)
SPOTS = ((0, 8), (8, 8), (16, 8), (24, 16), (40, 8))
BF16 = jnp.bfloat16
F32 = jnp.float32
ROWS = (2 * HOP + 1) * SPAN // LANES
PART = 16
SUBS = LANES // PART
WIDE = PART * SLOTS
REACH = 3 * LANES
CELLS = SUBS * ROWS
FAR = 248
MID = 184


GRANT = 24 << 20


def split(value):
    high = value.astype(BF16)
    low = (value - high.astype(F32)).astype(BF16)
    return high, low


def column(row):
    i = lax.broadcasted_iota(jnp.int32, (SLOTS, SLOTS), 0)
    j = lax.broadcasted_iota(jnp.int32, (SLOTS, SLOTS), 1)
    spread = jnp.where(i == j, jnp.broadcast_to(row, (SLOTS, SLOTS)), 0.0)
    return jnp.sum(spread, axis=1, keepdims=True)


def voigt_table(gauss_ref, lorentz_ref, mixing_ref, factor_ref, padded):
    padded[:, 0 : 2 * WING + 1] = factor_ref[...]
    back = LANES - 1 - lax.broadcasted_iota(jnp.int32, (SLOTS, LANES), 1)
    pieces = [
        jnp.take_along_axis(
            padded[:, c * LANES : (c + 1) * LANES], back, axis=1, mode="promise_in_bounds"
        )
        for c in (2, 1, 0)
    ]
    factor = jnp.concatenate(pieces, axis=1)
    m = lax.broadcasted_iota(jnp.int32, (SLOTS, REACH), 1)
    offset = (REACH - 1 - WING - m).astype(F32)
    square = offset * offset
    gauss_width = column(gauss_ref[...])
    lorentz_width = column(lorentz_ref[...])
    mixing = column(mixing_ref[...])
    wide = lorentz_width * lorentz_width
    lorentz = wide / (square + wide)
    gauss = jnp.exp(-square / (2.0 * gauss_width * gauss_width))
    raw = (mixing * lorentz + (1.0 - mixing) * gauss) * factor
    raw = jnp.where(m >= REACH - 1 - 2 * WING, raw, 0.0)
    return raw / jnp.sum(raw, axis=1, keepdims=True)


def conv(grid, t_high, t_low):
    rows = grid.shape[0]
    high = grid.astype(BF16).astype(F32)
    both = jnp.concatenate([high, grid - high], axis=0).astype(BF16)
    twice = jnp.dot(both, t_high[...], preferred_element_type=F32)
    rest = jnp.dot(high.astype(BF16), t_low[...], preferred_element_type=F32)
    return twice[0:rows] + twice[rows : 2 * rows] + rest


def kernel(
    n_grp,
    n_dev,
    bin_hbm,
    slot_hbm,
    strength_hbm,
    count_ref,
    gauss_hbm,
    lorentz_hbm,
    mixing_hbm,
    factor_hbm,
    own_ref,
    sum_ref,
    bin_ref,
    slot_ref,
    strength_ref,
    gauss_ref,
    lorentz_ref,
    mixing_ref,
    factor_ref,
    padded,
    t_high,
    t_low,
    wide_ref,
    stage,
    far,
    middle,
    near_up,
    near_down,
    lower,
    inbox,
    in_sem,
    send_sem,
    recv_sem,
    relay_sem,
):
    devices = n_grp * n_dev
    dev = lax.axis_index("dev")
    me = lax.axis_index("grp") * n_dev + dev

    loads = [
        pltpu.make_async_copy(source, target, in_sem.at[i])
        for i, (source, target) in enumerate(
            (
                (bin_hbm, bin_ref),
                (slot_hbm, slot_ref),
                (strength_hbm, strength_ref),
                (gauss_hbm, gauss_ref),
                (lorentz_hbm, lorentz_ref),
                (mixing_hbm, mixing_ref),
                (factor_hbm, factor_ref),
            )
        )
    ]
    for load in loads:
        load.start()
    z = lax.rem(dev, ROW)
    late = z >= ROW // 2

    def exists(o):
        return me + o < devices if o > 0 else me + o >= 0

    def tell(semaphore, condition, o):
        @pl.when(condition)
        def _():
            pl.semaphore_signal(
                semaphore,
                inc=1,
                device_id=(lax.div(me + o, n_dev), lax.rem(me + o, n_dev)),
                device_id_type=pl.DeviceIdType.MESH,
            )

    barrier = pltpu.get_barrier_semaphore()
    crosses = z >= ROW - 2
    heard = ((exists(2) & crosses) | (exists(-2) & (z == 0))).astype(jnp.int32)
    tell(barrier, exists(-2) & (z < 2), -2)
    tell(barrier, exists(2) & (z == ROW - 2), 2)
    for o in (3, 1, -1):
        heard = heard + exists(o).astype(jnp.int32)
        tell(barrier, exists(-o), -o)

    padded[...] = jnp.zeros((SLOTS, REACH), F32)
    for index, o in enumerate(OFFSETS):
        @pl.when(jnp.logical_not(exists(-o)))
        def _():
            at, rows = SPOTS[index]
            inbox[at : at + rows, :] = jnp.zeros((rows, LANES), F32)

    for load in loads[:3]:
        load.wait()

    lines = bin_ref.shape[0] * LANES
    near = bin_ref[...] - (dev - HOP) * SPAN
    slot = slot_ref[...]
    q = near // PART
    wide = (near % PART) * SLOTS + slot
    place = lax.broadcasted_iota(jnp.int32, near.shape, 0) * LANES + lax.broadcasted_iota(
        jnp.int32, near.shape, 1
    )
    weight = jnp.where(place < count_ref[0], strength_ref[...], 0.0)
    weight_high = weight.astype(BF16).astype(F32)
    weight_low = weight - weight_high
    wide = jnp.transpose(wide)
    for load in loads[3:]:
        load.wait()

    table = voigt_table(gauss_ref, lorentz_ref, mixing_ref, factor_ref, padded)
    table_high, table_low = split(table)
    for r in range(PART):
        rows = slice(r * SLOTS, (r + 1) * SLOTS)
        t_high[rows, :] = pltpu.roll(table_high, r + 2 * LANES + 1, 1)
        t_low[rows, :] = pltpu.roll(table_low, r + 2 * LANES + 1, 1)

    lane = lax.broadcasted_iota(jnp.int32, (LANES, LANES), 1)
    spot = lax.broadcasted_iota(jnp.int32, (16, LANES), 0)
    blocks = lines // LANES
    zero = jnp.zeros((16, LANES), BF16)

    def tile_of(value, k, dtype):
        return jnp.broadcast_to(value[k : k + 1, :], (16, LANES)).astype(dtype)

    wide_ref[...] = wide

    def columns(k):
        return jnp.broadcast_to(wide[:, k : k + 1], (LANES, LANES)).astype(jnp.int16)

    def kept(k):
        return jnp.broadcast_to(wide_ref[:, k : k + 1], (LANES, LANES)).astype(jnp.int16)

    def one_hot(column_of):
        rows = []
        for k in range(blocks):
            at = column_of(k)
            rows.append(
                jnp.concatenate(
                    [
                        jnp.where(
                            at == (lane + c * LANES).astype(jnp.int16),
                            jnp.ones((LANES, LANES), BF16),
                            jnp.zeros((LANES, LANES), BF16),
                        )
                        for c in range(WIDE // LANES)
                    ],
                    axis=1,
                )
            )
        return jnp.concatenate(rows, axis=0)

    def weighted(low_cell, high_cell):
        rows = high_cell - low_cell
        inside = jnp.logical_and(q >= low_cell, q < high_cell)
        place = jnp.where(inside, q - low_cell, -4 * CELLS)
        cols = []
        for k in range(blocks):
            at = tile_of(place, k, jnp.int16)
            at_low = tile_of(place + rows, k, jnp.int16)
            high = tile_of(weight_high, k, BF16)
            low = tile_of(weight_low, k, BF16)
            tiles = []
            for i in range(2 * rows // 16):
                here = (spot + i * 16).astype(jnp.int16)
                value = zero
                if (i + 1) * 16 > rows:
                    value = jnp.where(at_low == here, low, value)
                if i * 16 < rows:
                    value = jnp.where(at == here, high, value)
                tiles.append(value)
            cols.append(jnp.concatenate(tiles, axis=0))
        return jnp.concatenate(cols, axis=1)

    def deposit(low_cell, high_cell, column_of):
        rows = high_cell - low_cell
        both = jnp.dot(
            weighted(low_cell, high_cell), one_hot(column_of), preferred_element_type=F32
        )
        return both[0:rows] + both[rows : 2 * rows]

    def window(total):
        rows = total.shape[0] // SUBS
        for c in range(3):
            stage[c, 0 : total.shape[0], :] = total[:, c * LANES : (c + 1) * LANES]

        def every(sub):
            return jnp.concatenate(
                [stage[c, pl.ds(sub, rows, stride=SUBS), :] for c in range(3)], axis=1
            )

        value = every(0)
        for sub in range(1, SUBS):
            value = value + pltpu.roll(every(sub), sub * PART, 1)
        return value

    def spread(target, at, value):
        rows = value.shape[0]
        target[...] = jnp.zeros(target.shape, F32)
        target[at : at + rows, :] = value[:, 0:LANES]
        target[at + 1 : at + 1 + rows, :] += value[:, LANES : 2 * LANES]
        target[at + 2 : at + 2 + rows, :] += value[:, 2 * LANES : 3 * LANES]

    pieces = (far.at[pl.ds(16, 8), :], far.at[pl.ds(8, 8), :], near_up)
    pieces += (lower.at[pl.ds(0, 16), :], near_down)

    def copy(index):
        o = OFFSETS[index]
        return pltpu.make_async_remote_copy(
            src_ref=pieces[index],
            dst_ref=inbox.at[pl.ds(*SPOTS[index]), :],
            send_sem=send_sem.at[index],
            recv_sem=recv_sem.at[index],
            device_id=(lax.div(me + o, n_dev), lax.rem(me + o, n_dev)),
            device_id_type=pl.DeviceIdType.MESH,
        )

    def send(index, condition):
        @pl.when(jnp.logical_and(exists(OFFSETS[index]), condition))
        def _():
            copy(index).start()

    def greet(condition):
        @pl.when(condition)
        def _():
            pl.semaphore_wait(barrier, heard)

        tell(relay_sem.at[0], condition & (z > 0) & (z < ROW - 1), -1)
        tell(relay_sem.at[1], condition & exists(-1) & (z < ROW - 1), 1)

    spread(far, 6, window(conv(deposit(FAR, CELLS, columns), t_high, t_low)))
    greet(late)
    send(0, late)
    send(1, crosses)

    spread(middle, 6, window(conv(deposit(MID, FAR, kept), t_high, t_low)))
    near_up[...] = middle[8:16, :] + far[0:8, :]
    send(2, late)

    spread(lower, 7, window(conv(deposit(0, MID, kept), t_high, t_low)))
    own_ref[...] = lower[24:32, :] + middle[0:8, :]
    def take(index):
        @pl.when(exists(-OFFSETS[index]))
        def _():
            copy(index).wait_recv()

    greet(jnp.logical_not(late))
    send(0, jnp.logical_not(late))
    send(2, jnp.logical_not(late))

    def send_down(condition):
        @pl.when(condition & exists(-2) & (z > 0))
        def _():
            pl.semaphore_wait(relay_sem.at[1], 1)

        send(3, condition)

    send_down(z >= 2)
    take(3)
    near_down[...] = lower[16:24, :] + inbox[24:32, :]
    send(4, True)
    send_down(z < 2)

    @pl.when(jnp.logical_not(crosses))
    def _():
        pl.semaphore_wait(relay_sem.at[0], 1)

    send(1, jnp.logical_not(crosses))
    for index in (4, 2, 1, 0):
        take(index)

    total = inbox[0:8, :]
    for at in (8, 16, 32, 40):
        total = total + inbox[at : at + 8, :]
    sum_ref[...] = total
    for index, o in enumerate(OFFSETS):

        @pl.when(exists(o))
        def _():
            copy(index).wait_send()


def solution(mesh):
    n_grp, n_dev = mesh.shape["grp"], mesh.shape["dev"]

    def body(
        line_bin, line_slot, strength, line_count, gauss_width, lorentz_width, mixing, factor
    ):
        lines = line_bin.shape[0]

        def call(*refs):
            kernel(n_grp, n_dev, *refs)

        vmem = pl.BlockSpec(memory_space=pltpu.VMEM)
        hbm = pl.BlockSpec(memory_space=pltpu.HBM)
        piece = jax.ShapeDtypeStruct((SPAN // LANES, LANES), F32)
        own, received = pl.pallas_call(
            call,
            out_shape=(piece, piece),
            in_specs=[hbm] * 3 + [pl.BlockSpec(memory_space=pltpu.SMEM)] + [hbm] * 4,
            out_specs=(vmem, vmem),
            scratch_shapes=[
                pltpu.VMEM((lines // LANES, LANES), jnp.int32),
                pltpu.VMEM((lines // LANES, LANES), jnp.int32),
                pltpu.VMEM((lines // LANES, LANES), F32),
                pltpu.VMEM((1, SLOTS), F32),
                pltpu.VMEM((1, SLOTS), F32),
                pltpu.VMEM((1, SLOTS), F32),
                pltpu.VMEM((SLOTS, 2 * WING + 1), F32),
                pltpu.VMEM((SLOTS, REACH), F32),
                pltpu.VMEM((WIDE, REACH), BF16),
                pltpu.VMEM((WIDE, REACH), BF16),
                pltpu.VMEM((LANES, lines // LANES), jnp.int32),
                pltpu.VMEM((3, MID, LANES), F32),
                pltpu.VMEM((3 * 8, LANES), F32),
                pltpu.VMEM((2 * 8, LANES), F32),
                pltpu.VMEM((8, LANES), F32),
                pltpu.VMEM((8, LANES), F32),
                pltpu.VMEM((4 * 8, LANES), F32),
                pltpu.VMEM((6 * 8, LANES), F32),
                pltpu.SemaphoreType.DMA((7,)),
                pltpu.SemaphoreType.DMA((5,)),
                pltpu.SemaphoreType.DMA((5,)),
                pltpu.SemaphoreType.REGULAR((2,)),
            ],
            compiler_params=pltpu.CompilerParams(
                collective_id=0, has_side_effects=True, vmem_limit_bytes=GRANT
            ),
            name="voigt",
        )(
            *(
                value if value.size == 1 else pltpu.with_memory_space_constraint(value, pltpu.HBM)
                for value in (
                    line_bin.reshape(lines // LANES, LANES),
                    line_slot.reshape(lines // LANES, LANES),
                    strength.reshape(lines // LANES, LANES),
                    line_count,
                    gauss_width.reshape(1, SLOTS),
                    lorentz_width.reshape(1, SLOTS),
                    mixing.reshape(1, SLOTS),
                    factor,
                )
            )
        )
        return (own + received).reshape(SPAN)

    split_over = P(("grp", "dev"))
    return jax.shard_map(
        body,
        mesh=mesh,
        in_specs=(split_over,) * 4 + (P(),) * 4,
        out_specs=split_over,
        check_vma=False,
    )
```

```python
import jax
import jax.numpy as jnp
from jax import lax
from jax.experimental import pallas as pl
from jax.experimental.pallas import tpu as pltpu
from jax.sharding import PartitionSpec as P

SLOTS = 32
WING = 128
HOP = 2
SPAN = 1024
LANES = 128
ROW = 16
OFFSETS = (3, 2, 1, -2, -1)
SPOTS = ((0, 8), (8, 8), (16, 8), (24, 16), (40, 8))
BF16 = jnp.bfloat16
F32 = jnp.float32
ROWS = (2 * HOP + 1) * SPAN // LANES
PART = 16
SUBS = LANES // PART
WIDE = PART * SLOTS
REACH = 3 * LANES
CELLS = SUBS * ROWS
FAR = 248
MID = 184


GRANT = 24 << 20


def split(value):
    high = value.astype(BF16)
    low = (value - high.astype(F32)).astype(BF16)
    return high, low


def column(row):
    i = lax.broadcasted_iota(jnp.int32, (SLOTS, SLOTS), 0)
    j = lax.broadcasted_iota(jnp.int32, (SLOTS, SLOTS), 1)
    spread = jnp.where(i == j, jnp.broadcast_to(row, (SLOTS, SLOTS)), 0.0)
    return jnp.sum(spread, axis=1, keepdims=True)


def voigt_table(gauss_ref, lorentz_ref, mixing_ref, factor_ref, padded):
    padded[:, 0 : 2 * WING + 1] = factor_ref[...]
    back = LANES - 1 - lax.broadcasted_iota(jnp.int32, (SLOTS, LANES), 1)
    pieces = [
        jnp.take_along_axis(
            padded[:, c * LANES : (c + 1) * LANES], back, axis=1, mode="promise_in_bounds"
        )
        for c in (2, 1, 0)
    ]
    factor = jnp.concatenate(pieces, axis=1)
    m = lax.broadcasted_iota(jnp.int32, (SLOTS, REACH), 1)
    offset = (REACH - 1 - WING - m).astype(F32)
    square = offset * offset
    gauss_width = column(gauss_ref[...])
    lorentz_width = column(lorentz_ref[...])
    mixing = column(mixing_ref[...])
    wide = lorentz_width * lorentz_width
    lorentz = wide / (square + wide)
    gauss = jnp.exp(-square / (2.0 * gauss_width * gauss_width))
    raw = (mixing * lorentz + (1.0 - mixing) * gauss) * factor
    raw = jnp.where(m >= REACH - 1 - 2 * WING, raw, 0.0)
    return raw / jnp.sum(raw, axis=1, keepdims=True)


def conv(grid, t_high, t_low):
    rows = grid.shape[0]
    high = grid.astype(BF16).astype(F32)
    both = jnp.concatenate([high, grid - high], axis=0).astype(BF16)
    twice = jnp.dot(both, t_high[...], preferred_element_type=F32)
    rest = jnp.dot(high.astype(BF16), t_low[...], preferred_element_type=F32)
    return twice[0:rows] + twice[rows : 2 * rows] + rest


def kernel(
    n_grp,
    n_dev,
    bin_hbm,
    slot_hbm,
    strength_hbm,
    count_ref,
    gauss_hbm,
    lorentz_hbm,
    mixing_hbm,
    factor_hbm,
    own_ref,
    sum_ref,
    bin_ref,
    slot_ref,
    strength_ref,
    gauss_ref,
    lorentz_ref,
    mixing_ref,
    factor_ref,
    padded,
    t_high,
    t_low,
    wide_ref,
    stage,
    far,
    middle,
    near_up,
    near_down,
    lower,
    inbox,
    in_sem,
    send_sem,
    recv_sem,
    relay_sem,
):
    devices = n_grp * n_dev
    dev = lax.axis_index("dev")
    me = lax.axis_index("grp") * n_dev + dev

    loads = [
        pltpu.make_async_copy(source, target, in_sem.at[i])
        for i, (source, target) in enumerate(
            (
                (bin_hbm, bin_ref),
                (slot_hbm, slot_ref),
                (strength_hbm, strength_ref),
                (gauss_hbm, gauss_ref),
                (lorentz_hbm, lorentz_ref),
                (mixing_hbm, mixing_ref),
                (factor_hbm, factor_ref),
            )
        )
    ]
    for load in loads:
        load.start()
    z = lax.rem(dev, ROW)
    late = z >= ROW // 2

    def exists(o):
        return me + o < devices if o > 0 else me + o >= 0

    def tell(semaphore, condition, o):
        @pl.when(condition)
        def _():
            pl.semaphore_signal(
                semaphore,
                inc=1,
                device_id=(lax.div(me + o, n_dev), lax.rem(me + o, n_dev)),
                device_id_type=pl.DeviceIdType.MESH,
            )

    barrier = pltpu.get_barrier_semaphore()
    crosses = z >= ROW - 2
    heard = ((exists(2) & crosses) | (exists(-2) & (z == 0))).astype(jnp.int32)
    tell(barrier, exists(-2) & (z < 2), -2)
    tell(barrier, exists(2) & (z == ROW - 2), 2)
    for o in (3, 1, -1):
        heard = heard + exists(o).astype(jnp.int32)
        tell(barrier, exists(-o), -o)

    padded[...] = jnp.zeros((SLOTS, REACH), F32)
    for index, o in enumerate(OFFSETS):
        @pl.when(jnp.logical_not(exists(-o)))
        def _():
            at, rows = SPOTS[index]
            inbox[at : at + rows, :] = jnp.zeros((rows, LANES), F32)

    for load in loads[:3]:
        load.wait()

    lines = bin_ref.shape[0] * LANES
    near = bin_ref[...] - (dev - HOP) * SPAN
    slot = slot_ref[...]
    q = near // PART
    wide = (near % PART) * SLOTS + slot
    place = lax.broadcasted_iota(jnp.int32, near.shape, 0) * LANES + lax.broadcasted_iota(
        jnp.int32, near.shape, 1
    )
    weight = jnp.where(place < count_ref[0], strength_ref[...], 0.0)
    weight_high = weight.astype(BF16).astype(F32)
    weight_low = weight - weight_high
    wide = jnp.transpose(wide)
    for load in loads[3:]:
        load.wait()

    table = voigt_table(gauss_ref, lorentz_ref, mixing_ref, factor_ref, padded)
    table_high, table_low = split(table)
    for r in range(PART):
        rows = slice(r * SLOTS, (r + 1) * SLOTS)
        t_high[rows, :] = pltpu.roll(table_high, r + 2 * LANES + 1, 1)
        t_low[rows, :] = pltpu.roll(table_low, r + 2 * LANES + 1, 1)

    lane = lax.broadcasted_iota(jnp.int32, (LANES, LANES), 1)
    spot = lax.broadcasted_iota(jnp.int32, (16, LANES), 0)
    blocks = lines // LANES
    zero = jnp.zeros((16, LANES), BF16)

    def tile_of(value, k, dtype):
        return jnp.broadcast_to(value[k : k + 1, :], (16, LANES)).astype(dtype)

    pairs = wide[:, 0:(blocks // 2)] + wide[:, (blocks // 2) : 2 * (blocks // 2)] * 65536
    wide_ref[...] = pairs

    def unpack(words, k):
        word = words[:, k % (blocks // 2) : k % (blocks // 2) + 1]
        word = jnp.broadcast_to(word, (LANES, LANES))
        return (word if k < (blocks // 2) else word >> 16).astype(jnp.int16)

    def columns(k):
        return unpack(pairs, k)

    def kept(k):
        return unpack(wide_ref[...], k)

    def one_hot(column_of):
        rows = []
        for k in range(blocks):
            at = column_of(k)
            rows.append(
                jnp.concatenate(
                    [
                        jnp.where(
                            at == (lane + c * LANES).astype(jnp.int16),
                            jnp.ones((LANES, LANES), BF16),
                            jnp.zeros((LANES, LANES), BF16),
                        )
                        for c in range(WIDE // LANES)
                    ],
                    axis=1,
                )
            )
        return jnp.concatenate(rows, axis=0)

    def weighted(low_cell, high_cell):
        rows = high_cell - low_cell
        inside = jnp.logical_and(q >= low_cell, q < high_cell)
        place = jnp.where(inside, q - low_cell, -4 * CELLS)
        cols = []
        for k in range(blocks):
            at = tile_of(place, k, jnp.int16)
            at_low = tile_of(place + rows, k, jnp.int16)
            high = tile_of(weight_high, k, BF16)
            low = tile_of(weight_low, k, BF16)
            tiles = []
            for i in range(2 * rows // 16):
                here = (spot + i * 16).astype(jnp.int16)
                value = zero
                if (i + 1) * 16 > rows:
                    value = jnp.where(at_low == here, low, value)
                if i * 16 < rows:
                    value = jnp.where(at == here, high, value)
                tiles.append(value)
            cols.append(jnp.concatenate(tiles, axis=0))
        return jnp.concatenate(cols, axis=1)

    def deposit(low_cell, high_cell, column_of):
        rows = high_cell - low_cell
        both = jnp.dot(
            weighted(low_cell, high_cell), one_hot(column_of), preferred_element_type=F32
        )
        return both[0:rows] + both[rows : 2 * rows]

    def window(total):
        rows = total.shape[0] // SUBS
        for c in range(3):
            stage[c, 0 : total.shape[0], :] = total[:, c * LANES : (c + 1) * LANES]

        def every(sub):
            return jnp.concatenate(
                [stage[c, pl.ds(sub, rows, stride=SUBS), :] for c in range(3)], axis=1
            )

        value = every(0)
        for sub in range(1, SUBS):
            value = value + pltpu.roll(every(sub), sub * PART, 1)
        return value

    def spread(target, at, value):
        rows = value.shape[0]
        target[...] = jnp.zeros(target.shape, F32)
        target[at : at + rows, :] = value[:, 0:LANES]
        target[at + 1 : at + 1 + rows, :] += value[:, LANES : 2 * LANES]
        target[at + 2 : at + 2 + rows, :] += value[:, 2 * LANES : 3 * LANES]

    pieces = (far.at[pl.ds(16, 8), :], far.at[pl.ds(8, 8), :], near_up)
    pieces += (lower.at[pl.ds(0, 16), :], near_down)

    def copy(index):
        o = OFFSETS[index]
        return pltpu.make_async_remote_copy(
            src_ref=pieces[index],
            dst_ref=inbox.at[pl.ds(*SPOTS[index]), :],
            send_sem=send_sem.at[index],
            recv_sem=recv_sem.at[index],
            device_id=(lax.div(me + o, n_dev), lax.rem(me + o, n_dev)),
            device_id_type=pl.DeviceIdType.MESH,
        )

    def send(index, condition):
        @pl.when(jnp.logical_and(exists(OFFSETS[index]), condition))
        def _():
            copy(index).start()

    def greet(condition):
        @pl.when(condition)
        def _():
            pl.semaphore_wait(barrier, heard)

    def pass_on(condition):
        tell(relay_sem.at[0], condition & (z > 0) & (z < ROW - 1), -1)
        tell(relay_sem.at[1], condition & exists(-1) & (z < ROW - 1), 1)

    spread(far, 6, window(conv(deposit(FAR, CELLS, columns), t_high, t_low)))
    greet(late)
    send(0, late)
    send(1, crosses)
    pass_on(late)

    spread(middle, 6, window(conv(deposit(MID, FAR, kept), t_high, t_low)))
    near_up[...] = middle[8:16, :] + far[0:8, :]
    send(2, late)

    spread(lower, 7, window(conv(deposit(0, MID, kept), t_high, t_low)))
    own_ref[...] = lower[24:32, :] + middle[0:8, :]
    def take(index):
        @pl.when(exists(-OFFSETS[index]))
        def _():
            copy(index).wait_recv()

    greet(jnp.logical_not(late))
    send(0, jnp.logical_not(late))
    send(2, jnp.logical_not(late))
    pass_on(jnp.logical_not(late))

    def send_down(condition):
        @pl.when(condition & exists(-2) & (z > 0))
        def _():
            pl.semaphore_wait(relay_sem.at[1], 1)

        send(3, condition)

    send_down(z >= 2)
    take(3)
    near_down[...] = lower[16:24, :] + inbox[24:32, :]
    send(4, True)
    send_down(z < 2)

    @pl.when(jnp.logical_not(crosses))
    def _():
        pl.semaphore_wait(relay_sem.at[0], 1)

    send(1, jnp.logical_not(crosses))
    for index in (4, 2, 1, 0):
        take(index)

    total = inbox[0:8, :]
    for at in (8, 16, 32, 40):
        total = total + inbox[at : at + 8, :]
    sum_ref[...] = total
    for index, o in enumerate(OFFSETS):

        @pl.when(exists(o))
        def _():
            copy(index).wait_send()


def solution(mesh):
    n_grp, n_dev = mesh.shape["grp"], mesh.shape["dev"]

    def body(
        line_bin, line_slot, strength, line_count, gauss_width, lorentz_width, mixing, factor
    ):
        lines = line_bin.shape[0]

        def call(*refs):
            kernel(n_grp, n_dev, *refs)

        vmem = pl.BlockSpec(memory_space=pltpu.VMEM)
        hbm = pl.BlockSpec(memory_space=pltpu.HBM)
        piece = jax.ShapeDtypeStruct((SPAN // LANES, LANES), F32)
        own, received = pl.pallas_call(
            call,
            out_shape=(piece, piece),
            in_specs=[hbm] * 3 + [pl.BlockSpec(memory_space=pltpu.SMEM)] + [hbm] * 4,
            out_specs=(vmem, vmem),
            scratch_shapes=[
                pltpu.VMEM((lines // LANES, LANES), jnp.int32),
                pltpu.VMEM((lines // LANES, LANES), jnp.int32),
                pltpu.VMEM((lines // LANES, LANES), F32),
                pltpu.VMEM((1, SLOTS), F32),
                pltpu.VMEM((1, SLOTS), F32),
                pltpu.VMEM((1, SLOTS), F32),
                pltpu.VMEM((SLOTS, 2 * WING + 1), F32),
                pltpu.VMEM((SLOTS, REACH), F32),
                pltpu.VMEM((WIDE, REACH), BF16),
                pltpu.VMEM((WIDE, REACH), BF16),
                pltpu.VMEM((LANES, lines // LANES // 2), jnp.int32),
                pltpu.VMEM((3, MID, LANES), F32),
                pltpu.VMEM((3 * 8, LANES), F32),
                pltpu.VMEM((2 * 8, LANES), F32),
                pltpu.VMEM((8, LANES), F32),
                pltpu.VMEM((8, LANES), F32),
                pltpu.VMEM((4 * 8, LANES), F32),
                pltpu.VMEM((6 * 8, LANES), F32),
                pltpu.SemaphoreType.DMA((7,)),
                pltpu.SemaphoreType.DMA((5,)),
                pltpu.SemaphoreType.DMA((5,)),
                pltpu.SemaphoreType.REGULAR((2,)),
            ],
            compiler_params=pltpu.CompilerParams(
                collective_id=0, has_side_effects=True, vmem_limit_bytes=GRANT
            ),
            name="voigt",
        )(
            *(
                value if value.size == 1 else pltpu.with_memory_space_constraint(value, pltpu.HBM)
                for value in (
                    line_bin.reshape(lines // LANES, LANES),
                    line_slot.reshape(lines // LANES, LANES),
                    strength.reshape(lines // LANES, LANES),
                    line_count,
                    gauss_width.reshape(1, SLOTS),
                    lorentz_width.reshape(1, SLOTS),
                    mixing.reshape(1, SLOTS),
                    factor,
                )
            )
        )
        return (own + received).reshape(SPAN)

    split_over = P(("grp", "dev"))
    return jax.shard_map(
        body,
        mesh=mesh,
        in_specs=(split_over,) * 4 + (P(),) * 4,
        out_specs=split_over,
        check_vma=False,
    )
```

```python
import jax
import jax.numpy as jnp
from jax import lax
from jax.experimental import pallas as pl
from jax.experimental.pallas import tpu as pltpu
from jax.sharding import PartitionSpec as P

SLOTS = 32
WING = 128
HOP = 2
SPAN = 1024
LANES = 128
ROW = 16
OFFSETS = (3, 2, 1, -2, -1)
SPOTS = ((0, 8), (8, 8), (16, 8), (24, 16), (40, 8))
BF16 = jnp.bfloat16
F32 = jnp.float32
ROWS = (2 * HOP + 1) * SPAN // LANES
PART = 16
SUBS = LANES // PART
WIDE = PART * SLOTS
REACH = 3 * LANES
CELLS = SUBS * ROWS
FAR = 248
MID = 184


GRANT = 24 << 20


def split(value):
    high = value.astype(BF16)
    low = (value - high.astype(F32)).astype(BF16)
    return high, low


def column(row):
    i = lax.broadcasted_iota(jnp.int32, (SLOTS, SLOTS), 0)
    j = lax.broadcasted_iota(jnp.int32, (SLOTS, SLOTS), 1)
    spread = jnp.where(i == j, jnp.broadcast_to(row, (SLOTS, SLOTS)), 0.0)
    return jnp.sum(spread, axis=1, keepdims=True)


def voigt_table(gauss_ref, lorentz_ref, mixing_ref, factor_ref, padded):
    padded[:, 0 : 2 * WING + 1] = factor_ref[...]
    back = LANES - 1 - lax.broadcasted_iota(jnp.int32, (SLOTS, LANES), 1)
    pieces = [
        jnp.take_along_axis(
            padded[:, c * LANES : (c + 1) * LANES], back, axis=1, mode="promise_in_bounds"
        )
        for c in (2, 1, 0)
    ]
    factor = jnp.concatenate(pieces, axis=1)
    m = lax.broadcasted_iota(jnp.int32, (SLOTS, REACH), 1)
    offset = (REACH - 1 - WING - m).astype(F32)
    square = offset * offset
    gauss_width = column(gauss_ref[...])
    lorentz_width = column(lorentz_ref[...])
    mixing = column(mixing_ref[...])
    wide = lorentz_width * lorentz_width
    lorentz = wide / (square + wide)
    gauss = jnp.exp(-square / (2.0 * gauss_width * gauss_width))
    raw = (mixing * lorentz + (1.0 - mixing) * gauss) * factor
    raw = jnp.where(m >= REACH - 1 - 2 * WING, raw, 0.0)
    return raw / jnp.sum(raw, axis=1, keepdims=True)


def conv(grid, t_high, t_low):
    rows = grid.shape[0]
    high = grid.astype(BF16).astype(F32)
    both = jnp.concatenate([high, grid - high], axis=0).astype(BF16)
    twice = jnp.dot(both, t_high[...], preferred_element_type=F32)
    rest = jnp.dot(high.astype(BF16), t_low[...], preferred_element_type=F32)
    return twice[0:rows] + twice[rows : 2 * rows] + rest


def kernel(
    n_grp,
    n_dev,
    bin_hbm,
    slot_hbm,
    strength_hbm,
    count_ref,
    gauss_hbm,
    lorentz_hbm,
    mixing_hbm,
    factor_hbm,
    own_ref,
    sum_ref,
    bin_ref,
    slot_ref,
    strength_ref,
    gauss_ref,
    lorentz_ref,
    mixing_ref,
    factor_ref,
    padded,
    t_high,
    t_low,
    wide_ref,
    stage,
    far,
    middle,
    leak_ref,
    near_up,
    near_down,
    lower,
    inbox,
    in_sem,
    send_sem,
    recv_sem,
    relay_sem,
):
    devices = n_grp * n_dev
    dev = lax.axis_index("dev")
    me = lax.axis_index("grp") * n_dev + dev

    loads = [
        pltpu.make_async_copy(source, target, in_sem.at[i])
        for i, (source, target) in enumerate(
            (
                (bin_hbm, bin_ref),
                (slot_hbm, slot_ref),
                (strength_hbm, strength_ref),
                (gauss_hbm, gauss_ref),
                (lorentz_hbm, lorentz_ref),
                (mixing_hbm, mixing_ref),
                (factor_hbm, factor_ref),
            )
        )
    ]
    for load in loads:
        load.start()
    z = lax.rem(dev, ROW)
    late = z >= ROW // 2

    def exists(o):
        return me + o < devices if o > 0 else me + o >= 0

    def tell(semaphore, condition, o):
        @pl.when(condition)
        def _():
            pl.semaphore_signal(
                semaphore,
                inc=1,
                device_id=(lax.div(me + o, n_dev), lax.rem(me + o, n_dev)),
                device_id_type=pl.DeviceIdType.MESH,
            )

    barrier = pltpu.get_barrier_semaphore()
    crosses = z >= ROW - 2
    heard = ((exists(2) & crosses) | (exists(-2) & (z == 0))).astype(jnp.int32)
    tell(barrier, exists(-2) & (z < 2), -2)
    tell(barrier, exists(2) & (z == ROW - 2), 2)
    for o in (3, 1, -1):
        heard = heard + exists(o).astype(jnp.int32)
        tell(barrier, exists(-o), -o)

    padded[...] = jnp.zeros((SLOTS, REACH), F32)
    for index, o in enumerate(OFFSETS):
        @pl.when(jnp.logical_not(exists(-o)))
        def _():
            at, rows = SPOTS[index]
            inbox[at : at + rows, :] = jnp.zeros((rows, LANES), F32)

    for load in loads[:3]:
        load.wait()

    lines = bin_ref.shape[0] * LANES
    near = bin_ref[...] - (dev - HOP) * SPAN
    slot = slot_ref[...]
    q = near // PART
    wide = (near % PART) * SLOTS + slot
    place = lax.broadcasted_iota(jnp.int32, near.shape, 0) * LANES + lax.broadcasted_iota(
        jnp.int32, near.shape, 1
    )
    weight = jnp.where(place < count_ref[0], strength_ref[...], 0.0)
    weight_high = weight.astype(BF16).astype(F32)
    weight_low = weight - weight_high
    wide = jnp.transpose(wide)
    for load in loads[3:]:
        load.wait()

    lane = lax.broadcasted_iota(jnp.int32, (LANES, LANES), 1)
    spot = lax.broadcasted_iota(jnp.int32, (16, LANES), 0)
    blocks = lines // LANES
    zero = jnp.zeros((16, LANES), BF16)

    def tile_of(value, k, dtype):
        return jnp.broadcast_to(value[k : k + 1, :], (16, LANES)).astype(dtype)

    ahead = n_dev - dev
    pieces = (far.at[pl.ds(16, 8), :], far.at[pl.ds(8, 8), :], near_up)
    pieces += (lower.at[pl.ds(0, 16), :], near_down)

    def copy(index, source=None):
        o = OFFSETS[index]
        return pltpu.make_async_remote_copy(
            src_ref=pieces[index] if source is None else source,
            dst_ref=inbox.at[pl.ds(*SPOTS[index]), :],
            send_sem=send_sem.at[index],
            recv_sem=recv_sem.at[index],
            device_id=(lax.div(me + o, n_dev), lax.rem(me + o, n_dev)),
            device_id_type=pl.DeviceIdType.MESH,
        )

    def send(index, condition):
        o = OFFSETS[index]
        condition = jnp.logical_and(exists(o), condition)

        @pl.when(condition & (ahead != o) if o > 0 else condition)
        def _():
            copy(index).start()

    def leak():
        within = near - ((n_dev - dev + HOP) * SPAN - LANES)
        table_high, table_low = split(
            voigt_table(gauss_ref, lorentz_ref, mixing_ref, factor_ref, padded)
        )
        weights_high, weights_low, hits = [], [], []
        for k in range(blocks):
            bin_at = tile_of(within, k, jnp.int16)
            slot_at = tile_of(slot, k, jnp.int16)
            high = tile_of(weight_high, k, BF16)
            low = tile_of(weight_low, k, BF16)
            own = [slot_at == (spot + i * 16).astype(jnp.int16) for i in range(SLOTS // 16)]
            weights_high.append(jnp.concatenate([jnp.where(hit, high, zero) for hit in own], axis=0))
            weights_low.append(jnp.concatenate([jnp.where(hit, low, zero) for hit in own], axis=0))
            hits.append(
                jnp.concatenate(
                    [
                        jnp.where(
                            bin_at == (spot + i * 16).astype(jnp.int16),
                            jnp.ones((16, LANES), BF16),
                            zero,
                        )
                        for i in range(LANES // 16)
                    ],
                    axis=0,
                )
            )
        hits = jnp.concatenate(hits, axis=1)
        over_lines = (((1,), (1,)), ((), ()))
        grid = lax.dot_general(
            hits, jnp.concatenate(weights_high, axis=1), over_lines, preferred_element_type=F32
        ) + lax.dot_general(
            hits, jnp.concatenate(weights_low, axis=1), over_lines, preferred_element_type=F32
        )
        high, low = split(grid)
        kernel_high = table_high[:, 2 * LANES :]
        kernel_low = table_low[:, 2 * LANES :]
        spread_out = (
            jnp.dot(high, kernel_high, preferred_element_type=F32)
            + jnp.dot(low, kernel_high, preferred_element_type=F32)
            + jnp.dot(high, kernel_low, preferred_element_type=F32)
        )
        moved = pltpu.roll(spread_out, 1, 1, stride=1, stride_axis=0)
        row = lax.broadcasted_iota(jnp.int32, (LANES, LANES), 0)
        return jnp.sum(jnp.where(lane <= row, moved, 0.0), axis=0, keepdims=True)

    edge = (ahead <= 3) & (me + ahead < devices)

    @pl.when(edge)
    def _():
        leak_ref[...] = jnp.zeros((8, LANES), F32)
        leak_ref[0:1, :] = leak()
        pl.semaphore_wait(barrier, heard)
        for index in range(3):

            @pl.when(ahead == OFFSETS[index])
            def _():
                copy(index, leak_ref).start()

    table = voigt_table(gauss_ref, lorentz_ref, mixing_ref, factor_ref, padded)
    table_high, table_low = split(table)
    for r in range(PART):
        rows = slice(r * SLOTS, (r + 1) * SLOTS)
        t_high[rows, :] = pltpu.roll(table_high, r + 2 * LANES + 1, 1)
        t_low[rows, :] = pltpu.roll(table_low, r + 2 * LANES + 1, 1)

    pairs = wide[:, 0:(blocks // 2)] + wide[:, (blocks // 2) : 2 * (blocks // 2)] * 65536
    wide_ref[...] = pairs

    def unpack(words, k):
        word = words[:, k % (blocks // 2) : k % (blocks // 2) + 1]
        word = jnp.broadcast_to(word, (LANES, LANES))
        return (word if k < (blocks // 2) else word >> 16).astype(jnp.int16)

    def columns(k):
        return unpack(pairs, k)

    def kept(k):
        return unpack(wide_ref[...], k)

    def one_hot(column_of):
        rows = []
        for k in range(blocks):
            at = column_of(k)
            rows.append(
                jnp.concatenate(
                    [
                        jnp.where(
                            at == (lane + c * LANES).astype(jnp.int16),
                            jnp.ones((LANES, LANES), BF16),
                            jnp.zeros((LANES, LANES), BF16),
                        )
                        for c in range(WIDE // LANES)
                    ],
                    axis=1,
                )
            )
        return jnp.concatenate(rows, axis=0)

    def weighted(low_cell, high_cell):
        rows = high_cell - low_cell
        inside = jnp.logical_and(q >= low_cell, q < high_cell)
        place = jnp.where(inside, q - low_cell, -4 * CELLS)
        cols = []
        for k in range(blocks):
            at = tile_of(place, k, jnp.int16)
            at_low = tile_of(place + rows, k, jnp.int16)
            high = tile_of(weight_high, k, BF16)
            low = tile_of(weight_low, k, BF16)
            tiles = []
            for i in range(2 * rows // 16):
                here = (spot + i * 16).astype(jnp.int16)
                value = zero
                if (i + 1) * 16 > rows:
                    value = jnp.where(at_low == here, low, value)
                if i * 16 < rows:
                    value = jnp.where(at == here, high, value)
                tiles.append(value)
            cols.append(jnp.concatenate(tiles, axis=0))
        return jnp.concatenate(cols, axis=1)

    def deposit(low_cell, high_cell, column_of):
        rows = high_cell - low_cell
        both = jnp.dot(
            weighted(low_cell, high_cell), one_hot(column_of), preferred_element_type=F32
        )
        return both[0:rows] + both[rows : 2 * rows]

    def window(total):
        rows = total.shape[0] // SUBS
        for c in range(3):
            stage[c, 0 : total.shape[0], :] = total[:, c * LANES : (c + 1) * LANES]

        def every(sub):
            return jnp.concatenate(
                [stage[c, pl.ds(sub, rows, stride=SUBS), :] for c in range(3)], axis=1
            )

        value = every(0)
        for sub in range(1, SUBS):
            value = value + pltpu.roll(every(sub), sub * PART, 1)
        return value

    def spread(target, at, value):
        rows = value.shape[0]
        target[...] = jnp.zeros(target.shape, F32)
        target[at : at + rows, :] = value[:, 0:LANES]
        target[at + 1 : at + 1 + rows, :] += value[:, LANES : 2 * LANES]
        target[at + 2 : at + 2 + rows, :] += value[:, 2 * LANES : 3 * LANES]

    def greet(condition):
        @pl.when(condition)
        def _():
            pl.semaphore_wait(barrier, heard)

    def pass_on(condition):
        tell(relay_sem.at[0], condition & (z > 0) & (z < ROW - 1), -1)
        tell(relay_sem.at[1], condition & exists(-1) & (z < ROW - 1), 1)

    spread(far, 6, window(conv(deposit(FAR, CELLS, columns), t_high, t_low)))
    greet(late & jnp.logical_not(edge))
    send(0, late)
    send(1, crosses)
    pass_on(late)

    spread(middle, 6, window(conv(deposit(MID, FAR, kept), t_high, t_low)))
    near_up[...] = middle[8:16, :] + far[0:8, :]
    send(2, late)

    spread(lower, 7, window(conv(deposit(0, MID, kept), t_high, t_low)))
    own_ref[...] = lower[24:32, :] + middle[0:8, :]
    def take(index):
        @pl.when(exists(-OFFSETS[index]))
        def _():
            copy(index).wait_recv()

    greet(jnp.logical_not(late))
    send(0, jnp.logical_not(late))
    send(2, jnp.logical_not(late))
    pass_on(jnp.logical_not(late))

    def send_down(condition):
        @pl.when(condition & exists(-2) & (z > 0))
        def _():
            pl.semaphore_wait(relay_sem.at[1], 1)

        send(3, condition)

    send_down(z >= 2)
    take(3)
    near_down[...] = lower[16:24, :] + inbox[24:32, :]
    send(4, True)
    send_down(z < 2)

    @pl.when(jnp.logical_not(crosses))
    def _():
        pl.semaphore_wait(relay_sem.at[0], 1)

    send(1, jnp.logical_not(crosses))
    for index in (4, 2, 1, 0):
        take(index)

    total = inbox[0:8, :]
    for at in (8, 16, 32, 40):
        total = total + inbox[at : at + 8, :]
    sum_ref[...] = total
    for index, o in enumerate(OFFSETS):

        @pl.when(exists(o))
        def _():
            copy(index).wait_send()


def solution(mesh):
    n_grp, n_dev = mesh.shape["grp"], mesh.shape["dev"]

    def body(
        line_bin, line_slot, strength, line_count, gauss_width, lorentz_width, mixing, factor
    ):
        lines = line_bin.shape[0]

        def call(*refs):
            kernel(n_grp, n_dev, *refs)

        vmem = pl.BlockSpec(memory_space=pltpu.VMEM)
        hbm = pl.BlockSpec(memory_space=pltpu.HBM)
        piece = jax.ShapeDtypeStruct((SPAN // LANES, LANES), F32)
        own, received = pl.pallas_call(
            call,
            out_shape=(piece, piece),
            in_specs=[hbm] * 3 + [pl.BlockSpec(memory_space=pltpu.SMEM)] + [hbm] * 4,
            out_specs=(vmem, vmem),
            scratch_shapes=[
                pltpu.VMEM((lines // LANES, LANES), jnp.int32),
                pltpu.VMEM((lines // LANES, LANES), jnp.int32),
                pltpu.VMEM((lines // LANES, LANES), F32),
                pltpu.VMEM((1, SLOTS), F32),
                pltpu.VMEM((1, SLOTS), F32),
                pltpu.VMEM((1, SLOTS), F32),
                pltpu.VMEM((SLOTS, 2 * WING + 1), F32),
                pltpu.VMEM((SLOTS, REACH), F32),
                pltpu.VMEM((WIDE, REACH), BF16),
                pltpu.VMEM((WIDE, REACH), BF16),
                pltpu.VMEM((LANES, lines // LANES // 2), jnp.int32),
                pltpu.VMEM((3, MID, LANES), F32),
                pltpu.VMEM((3 * 8, LANES), F32),
                pltpu.VMEM((2 * 8, LANES), F32),
                pltpu.VMEM((8, LANES), F32),
                pltpu.VMEM((8, LANES), F32),
                pltpu.VMEM((8, LANES), F32),
                pltpu.VMEM((4 * 8, LANES), F32),
                pltpu.VMEM((6 * 8, LANES), F32),
                pltpu.SemaphoreType.DMA((7,)),
                pltpu.SemaphoreType.DMA((5,)),
                pltpu.SemaphoreType.DMA((5,)),
                pltpu.SemaphoreType.REGULAR((2,)),
            ],
            compiler_params=pltpu.CompilerParams(
                collective_id=0, has_side_effects=True, vmem_limit_bytes=GRANT
            ),
            name="voigt",
        )(
            *(
                value if value.size == 1 else pltpu.with_memory_space_constraint(value, pltpu.HBM)
                for value in (
                    line_bin.reshape(lines // LANES, LANES),
                    line_slot.reshape(lines // LANES, LANES),
                    strength.reshape(lines // LANES, LANES),
                    line_count,
                    gauss_width.reshape(1, SLOTS),
                    lorentz_width.reshape(1, SLOTS),
                    mixing.reshape(1, SLOTS),
                    factor,
                )
            )
        )
        return (own + received).reshape(SPAN)

    split_over = P(("grp", "dev"))
    return jax.shard_map(
        body,
        mesh=mesh,
        in_specs=(split_over,) * 4 + (P(),) * 4,
        out_specs=split_over,
        check_vma=False,
    )
```

```python
import jax
import jax.numpy as jnp
from jax import lax
from jax.experimental import pallas as pl
from jax.experimental.pallas import tpu as pltpu
from jax.sharding import PartitionSpec as P

SLOTS = 32
WING = 128
HOP = 2
SPAN = 1024
LANES = 128
ROW = 16
OFFSETS = (3, 2, 1, -2, -1)
SPOTS = ((0, 8), (8, 8), (16, 8), (24, 16), (40, 8))
BF16 = jnp.bfloat16
F32 = jnp.float32
ROWS = (2 * HOP + 1) * SPAN // LANES
PART = 16
SUBS = LANES // PART
WIDE = PART * SLOTS
REACH = 3 * LANES
CELLS = SUBS * ROWS
FAR = 248
MID = 184


GRANT = 24 << 20


def split(value):
    high = value.astype(BF16)
    low = (value - high.astype(F32)).astype(BF16)
    return high, low


def column(row):
    i = lax.broadcasted_iota(jnp.int32, (SLOTS, SLOTS), 0)
    j = lax.broadcasted_iota(jnp.int32, (SLOTS, SLOTS), 1)
    spread = jnp.where(i == j, jnp.broadcast_to(row, (SLOTS, SLOTS)), 0.0)
    return jnp.sum(spread, axis=1, keepdims=True)


def voigt_table(gauss_ref, lorentz_ref, mixing_ref, factor_ref, padded):
    padded[:, 0 : 2 * WING + 1] = factor_ref[...]
    back = LANES - 1 - lax.broadcasted_iota(jnp.int32, (SLOTS, LANES), 1)
    pieces = [
        jnp.take_along_axis(
            padded[:, c * LANES : (c + 1) * LANES], back, axis=1, mode="promise_in_bounds"
        )
        for c in (2, 1, 0)
    ]
    factor = jnp.concatenate(pieces, axis=1)
    m = lax.broadcasted_iota(jnp.int32, (SLOTS, REACH), 1)
    offset = (REACH - 1 - WING - m).astype(F32)
    square = offset * offset
    gauss_width = column(gauss_ref[...])
    lorentz_width = column(lorentz_ref[...])
    mixing = column(mixing_ref[...])
    wide = lorentz_width * lorentz_width
    lorentz = wide / (square + wide)
    gauss = jnp.exp(-square / (2.0 * gauss_width * gauss_width))
    raw = (mixing * lorentz + (1.0 - mixing) * gauss) * factor
    raw = jnp.where(m >= REACH - 1 - 2 * WING, raw, 0.0)
    return raw / jnp.sum(raw, axis=1, keepdims=True)


def conv(grid, t_high, t_low):
    rows = grid.shape[0]
    high = grid.astype(BF16).astype(F32)
    both = jnp.concatenate([high, grid - high], axis=0).astype(BF16)
    twice = jnp.dot(both, t_high[...], preferred_element_type=F32)
    rest = jnp.dot(high.astype(BF16), t_low[...], preferred_element_type=F32)
    return twice[0:rows] + twice[rows : 2 * rows] + rest


def kernel(
    n_grp,
    n_dev,
    bin_hbm,
    slot_hbm,
    strength_hbm,
    count_ref,
    gauss_hbm,
    lorentz_hbm,
    mixing_hbm,
    factor_hbm,
    own_ref,
    sum_ref,
    bin_ref,
    slot_ref,
    strength_ref,
    gauss_ref,
    lorentz_ref,
    mixing_ref,
    factor_ref,
    padded,
    t_high,
    t_low,
    wide_ref,
    stage,
    far,
    middle,
    leak_ref,
    near_up,
    near_down,
    lower,
    inbox,
    in_sem,
    send_sem,
    recv_sem,
    relay_sem,
):
    devices = n_grp * n_dev
    dev = lax.axis_index("dev")
    me = lax.axis_index("grp") * n_dev + dev

    loads = [
        pltpu.make_async_copy(source, target, in_sem.at[i])
        for i, (source, target) in enumerate(
            (
                (bin_hbm, bin_ref),
                (slot_hbm, slot_ref),
                (strength_hbm, strength_ref),
                (gauss_hbm, gauss_ref),
                (lorentz_hbm, lorentz_ref),
                (mixing_hbm, mixing_ref),
                (factor_hbm, factor_ref),
            )
        )
    ]
    for load in loads:
        load.start()
    z = lax.rem(dev, ROW)
    late = z >= ROW // 2

    def exists(o):
        return me + o < devices if o > 0 else me + o >= 0

    def tell(semaphore, condition, o):
        @pl.when(condition)
        def _():
            pl.semaphore_signal(
                semaphore,
                inc=1,
                device_id=(lax.div(me + o, n_dev), lax.rem(me + o, n_dev)),
                device_id_type=pl.DeviceIdType.MESH,
            )

    barrier = pltpu.get_barrier_semaphore()
    crosses = z >= ROW - 2
    heard = ((exists(2) & crosses) | (exists(-2) & (z == 0))).astype(jnp.int32)
    tell(barrier, exists(-2) & (z < 2), -2)
    tell(barrier, exists(2) & (z == ROW - 2), 2)
    for o in (3, 1, -1):
        heard = heard + exists(o).astype(jnp.int32)
        tell(barrier, exists(-o), -o)

    padded[...] = jnp.zeros((SLOTS, REACH), F32)
    for index, o in enumerate(OFFSETS):
        @pl.when(jnp.logical_not(exists(-o)))
        def _():
            at, rows = SPOTS[index]
            inbox[at : at + rows, :] = jnp.zeros((rows, LANES), F32)

        if o > 0:

            @pl.when(exists(-o) & (dev == 0))
            def _():
                at, rows = SPOTS[index]
                inbox[at + 1 : at + rows, :] = jnp.zeros((rows - 1, LANES), F32)

    for load in loads[:3]:
        load.wait()

    lines = bin_ref.shape[0] * LANES
    near = bin_ref[...] - (dev - HOP) * SPAN
    slot = slot_ref[...]
    q = near // PART
    wide = (near % PART) * SLOTS + slot
    place = lax.broadcasted_iota(jnp.int32, near.shape, 0) * LANES + lax.broadcasted_iota(
        jnp.int32, near.shape, 1
    )
    weight = jnp.where(place < count_ref[0], strength_ref[...], 0.0)
    weight_high = weight.astype(BF16).astype(F32)
    weight_low = weight - weight_high
    wide = jnp.transpose(wide)
    for load in loads[3:]:
        load.wait()

    lane = lax.broadcasted_iota(jnp.int32, (LANES, LANES), 1)
    spot = lax.broadcasted_iota(jnp.int32, (16, LANES), 0)
    blocks = lines // LANES
    zero = jnp.zeros((16, LANES), BF16)

    def tile_of(value, k, dtype):
        return jnp.broadcast_to(value[k : k + 1, :], (16, LANES)).astype(dtype)

    ahead = n_dev - dev
    pieces = (far.at[pl.ds(16, 8), :], far.at[pl.ds(8, 8), :], near_up)
    pieces += (lower.at[pl.ds(0, 16), :], near_down)

    def copy(index, source=None):
        at, rows = SPOTS[index] if source is None else (SPOTS[index][0], 1)
        o = OFFSETS[index]
        return pltpu.make_async_remote_copy(
            src_ref=pieces[index] if source is None else source,
            dst_ref=inbox.at[pl.ds(at, rows), :],
            send_sem=send_sem.at[index],
            recv_sem=recv_sem.at[index],
            device_id=(lax.div(me + o, n_dev), lax.rem(me + o, n_dev)),
            device_id_type=pl.DeviceIdType.MESH,
        )

    def send(index, condition):
        o = OFFSETS[index]
        condition = jnp.logical_and(exists(o), condition)

        @pl.when(condition & (ahead != o) if o > 0 else condition)
        def _():
            copy(index).start()

    def leak():
        within = near - ((n_dev - dev + HOP) * SPAN - LANES)
        table_high, table_low = split(
            voigt_table(gauss_ref, lorentz_ref, mixing_ref, factor_ref, padded)
        )
        weights, hits = [], []
        for k in range(blocks):
            bin_at = tile_of(within, k, jnp.int16)
            slot_at = tile_of(slot, k, jnp.int16)
            high = tile_of(weight_high, k, BF16)
            low = tile_of(weight_low, k, BF16)
            own = [slot_at == (spot + i * 16).astype(jnp.int16) for i in range(SLOTS // 16)]
            weights.append(
                jnp.concatenate(
                    [jnp.where(hit, part, zero) for part in (high, low) for hit in own], axis=0
                )
            )
            hits.append(
                jnp.concatenate(
                    [
                        jnp.where(
                            bin_at == (spot + i * 16).astype(jnp.int16),
                            jnp.ones((16, LANES), BF16),
                            zero,
                        )
                        for i in range(LANES // 16)
                    ],
                    axis=0,
                )
            )
        hits = jnp.concatenate(hits, axis=1)
        grid = lax.dot_general(
            hits,
            jnp.concatenate(weights, axis=1),
            (((1,), (1,)), ((), ())),
            preferred_element_type=F32,
        )
        high, low = split(grid)
        kernel_high = jnp.concatenate([table_high[:, 2 * LANES :]] * 2, axis=0)
        kernel_low = jnp.concatenate([table_low[:, 2 * LANES :]] * 2, axis=0)
        spread_out = (
            jnp.dot(high, kernel_high, preferred_element_type=F32)
            + jnp.dot(low, kernel_high, preferred_element_type=F32)
            + jnp.dot(high, kernel_low, preferred_element_type=F32)
        )
        moved = pltpu.roll(spread_out, 1, 1, stride=1, stride_axis=0)
        row = lax.broadcasted_iota(jnp.int32, (LANES, LANES), 0)
        return jnp.sum(jnp.where(lane <= row, moved, 0.0), axis=0, keepdims=True)

    edge = (ahead <= 3) & (me + ahead < devices)

    @pl.when(edge)
    def _():
        leak_ref[...] = leak()
        pl.semaphore_wait(barrier, heard)
        for index in range(3):

            @pl.when(ahead == OFFSETS[index])
            def _():
                copy(index, leak_ref).start()

    table = voigt_table(gauss_ref, lorentz_ref, mixing_ref, factor_ref, padded)
    table_high, table_low = split(table)
    for r in range(PART):
        rows = slice(r * SLOTS, (r + 1) * SLOTS)
        t_high[rows, :] = pltpu.roll(table_high, r + 2 * LANES + 1, 1)
        t_low[rows, :] = pltpu.roll(table_low, r + 2 * LANES + 1, 1)

    pairs = wide[:, 0:(blocks // 2)] + wide[:, (blocks // 2) : 2 * (blocks // 2)] * 65536
    wide_ref[...] = pairs

    def unpack(words, k):
        word = words[:, k % (blocks // 2) : k % (blocks // 2) + 1]
        word = jnp.broadcast_to(word, (LANES, LANES))
        return (word if k < (blocks // 2) else word >> 16).astype(jnp.int16)

    def columns(k):
        return unpack(pairs, k)

    def kept(k):
        return unpack(wide_ref[...], k)

    def one_hot(column_of):
        rows = []
        for k in range(blocks):
            at = column_of(k)
            rows.append(
                jnp.concatenate(
                    [
                        jnp.where(
                            at == (lane + c * LANES).astype(jnp.int16),
                            jnp.ones((LANES, LANES), BF16),
                            jnp.zeros((LANES, LANES), BF16),
                        )
                        for c in range(WIDE // LANES)
                    ],
                    axis=1,
                )
            )
        return jnp.concatenate(rows, axis=0)

    def weighted(low_cell, high_cell):
        rows = high_cell - low_cell
        inside = jnp.logical_and(q >= low_cell, q < high_cell)
        place = jnp.where(inside, q - low_cell, -4 * CELLS)
        cols = []
        for k in range(blocks):
            at = tile_of(place, k, jnp.int16)
            at_low = tile_of(place + rows, k, jnp.int16)
            high = tile_of(weight_high, k, BF16)
            low = tile_of(weight_low, k, BF16)
            tiles = []
            for i in range(2 * rows // 16):
                here = (spot + i * 16).astype(jnp.int16)
                value = zero
                if (i + 1) * 16 > rows:
                    value = jnp.where(at_low == here, low, value)
                if i * 16 < rows:
                    value = jnp.where(at == here, high, value)
                tiles.append(value)
            cols.append(jnp.concatenate(tiles, axis=0))
        return jnp.concatenate(cols, axis=1)

    def deposit(low_cell, high_cell, column_of):
        rows = high_cell - low_cell
        both = jnp.dot(
            weighted(low_cell, high_cell), one_hot(column_of), preferred_element_type=F32
        )
        return both[0:rows] + both[rows : 2 * rows]

    def window(total):
        rows = total.shape[0] // SUBS
        for c in range(3):
            stage[c, 0 : total.shape[0], :] = total[:, c * LANES : (c + 1) * LANES]

        def every(sub):
            return jnp.concatenate(
                [stage[c, pl.ds(sub, rows, stride=SUBS), :] for c in range(3)], axis=1
            )

        value = every(0)
        for sub in range(1, SUBS):
            value = value + pltpu.roll(every(sub), sub * PART, 1)
        return value

    def spread(target, at, value):
        rows = value.shape[0]
        target[...] = jnp.zeros(target.shape, F32)
        target[at : at + rows, :] = value[:, 0:LANES]
        target[at + 1 : at + 1 + rows, :] += value[:, LANES : 2 * LANES]
        target[at + 2 : at + 2 + rows, :] += value[:, 2 * LANES : 3 * LANES]

    def greet(condition):
        @pl.when(condition)
        def _():
            pl.semaphore_wait(barrier, heard)

    def pass_on(condition):
        tell(relay_sem.at[0], condition & (z > 0) & (z < ROW - 1), -1)
        tell(relay_sem.at[1], condition & exists(-1) & (z < ROW - 1), 1)

    spread(far, 6, window(conv(deposit(FAR, CELLS, columns), t_high, t_low)))
    greet(late & jnp.logical_not(edge))
    send(0, late)
    send(1, crosses)
    pass_on(late)

    spread(middle, 6, window(conv(deposit(MID, FAR, kept), t_high, t_low)))
    near_up[...] = middle[8:16, :] + far[0:8, :]
    send(2, late)

    spread(lower, 7, window(conv(deposit(0, MID, kept), t_high, t_low)))
    own_ref[...] = lower[24:32, :] + middle[0:8, :]
    def leaks(o):
        return exists(-o) & (dev == 0) if o > 0 else me < 0

    def take(index):
        o = OFFSETS[index]

        @pl.when(exists(-o) & jnp.logical_not(leaks(o)))
        def _():
            copy(index).wait_recv()

        if o > 0:

            @pl.when(leaks(o))
            def _():
                copy(index, leak_ref).wait_recv()

    greet(jnp.logical_not(late))
    send(0, jnp.logical_not(late))
    send(2, jnp.logical_not(late))
    pass_on(jnp.logical_not(late))

    def send_down(condition):
        @pl.when(condition & exists(-2) & (z > 0))
        def _():
            pl.semaphore_wait(relay_sem.at[1], 1)

        send(3, condition)

    send_down(z >= 2)
    take(3)
    near_down[...] = lower[16:24, :] + inbox[24:32, :]
    send(4, True)
    send_down(z < 2)

    @pl.when(jnp.logical_not(crosses))
    def _():
        pl.semaphore_wait(relay_sem.at[0], 1)

    send(1, jnp.logical_not(crosses))
    for index in (4, 2, 1, 0):
        take(index)

    total = inbox[0:8, :]
    for at in (8, 16, 32, 40):
        total = total + inbox[at : at + 8, :]
    sum_ref[...] = total
    for index, o in enumerate(OFFSETS):

        @pl.when(exists(o) & jnp.logical_not(edge & (ahead == o)))
        def _():
            copy(index).wait_send()

        if o > 0:

            @pl.when(edge & (ahead == o))
            def _():
                copy(index, leak_ref).wait_send()


def solution(mesh):
    n_grp, n_dev = mesh.shape["grp"], mesh.shape["dev"]

    def body(
        line_bin, line_slot, strength, line_count, gauss_width, lorentz_width, mixing, factor
    ):
        lines = line_bin.shape[0]

        def call(*refs):
            kernel(n_grp, n_dev, *refs)

        vmem = pl.BlockSpec(memory_space=pltpu.VMEM)
        hbm = pl.BlockSpec(memory_space=pltpu.HBM)
        piece = jax.ShapeDtypeStruct((SPAN // LANES, LANES), F32)
        own, received = pl.pallas_call(
            call,
            out_shape=(piece, piece),
            in_specs=[hbm] * 3 + [pl.BlockSpec(memory_space=pltpu.SMEM)] + [hbm] * 4,
            out_specs=(vmem, vmem),
            scratch_shapes=[
                pltpu.VMEM((lines // LANES, LANES), jnp.int32),
                pltpu.VMEM((lines // LANES, LANES), jnp.int32),
                pltpu.VMEM((lines // LANES, LANES), F32),
                pltpu.VMEM((1, SLOTS), F32),
                pltpu.VMEM((1, SLOTS), F32),
                pltpu.VMEM((1, SLOTS), F32),
                pltpu.VMEM((SLOTS, 2 * WING + 1), F32),
                pltpu.VMEM((SLOTS, REACH), F32),
                pltpu.VMEM((WIDE, REACH), BF16),
                pltpu.VMEM((WIDE, REACH), BF16),
                pltpu.VMEM((LANES, lines // LANES // 2), jnp.int32),
                pltpu.VMEM((3, MID, LANES), F32),
                pltpu.VMEM((3 * 8, LANES), F32),
                pltpu.VMEM((2 * 8, LANES), F32),
                pltpu.VMEM((1, LANES), F32),
                pltpu.VMEM((8, LANES), F32),
                pltpu.VMEM((8, LANES), F32),
                pltpu.VMEM((4 * 8, LANES), F32),
                pltpu.VMEM((6 * 8, LANES), F32),
                pltpu.SemaphoreType.DMA((7,)),
                pltpu.SemaphoreType.DMA((5,)),
                pltpu.SemaphoreType.DMA((5,)),
                pltpu.SemaphoreType.REGULAR((2,)),
            ],
            compiler_params=pltpu.CompilerParams(
                collective_id=0,
                has_side_effects=True,
                vmem_limit_bytes=GRANT,
            ),
            name="voigt",
        )(
            *(
                value if value.size == 1 else pltpu.with_memory_space_constraint(value, pltpu.HBM)
                for value in (
                    line_bin.reshape(lines // LANES, LANES),
                    line_slot.reshape(lines // LANES, LANES),
                    strength.reshape(lines // LANES, LANES),
                    line_count,
                    gauss_width.reshape(1, SLOTS),
                    lorentz_width.reshape(1, SLOTS),
                    mixing.reshape(1, SLOTS),
                    factor,
                )
            )
        )
        return (own + received).reshape(SPAN)

    split_over = P(("grp", "dev"))
    return jax.shard_map(
        body,
        mesh=mesh,
        in_specs=(split_over,) * 4 + (P(),) * 4,
        out_specs=split_over,
        check_vma=False,
    )
```

```python
import jax
import jax.numpy as jnp
from jax import lax
from jax.experimental import pallas as pl
from jax.experimental.pallas import tpu as pltpu
from jax.sharding import PartitionSpec as P

SLOTS = 32
WING = 128
HOP = 2
SPAN = 1024
LANES = 128
ROW = 16
OFFSETS = (3, 2, 1, -2, -1)
SPOTS = ((0, 8), (8, 8), (16, 8), (24, 16), (40, 8))
BF16 = jnp.bfloat16
F32 = jnp.float32
ROWS = (2 * HOP + 1) * SPAN // LANES
PART = 16
SUBS = LANES // PART
WIDE = PART * SLOTS
REACH = 3 * LANES
CELLS = SUBS * ROWS
FAR = 248
MID = 184


GRANT = 24 << 20


def split(value):
    high = value.astype(BF16)
    low = (value - high.astype(F32)).astype(BF16)
    return high, low


def column(row):
    i = lax.broadcasted_iota(jnp.int32, (SLOTS, SLOTS), 0)
    j = lax.broadcasted_iota(jnp.int32, (SLOTS, SLOTS), 1)
    spread = jnp.where(i == j, jnp.broadcast_to(row, (SLOTS, SLOTS)), 0.0)
    return jnp.sum(spread, axis=1, keepdims=True)


def voigt_table(gauss_ref, lorentz_ref, mixing_ref, factor_ref, padded):
    padded[:, 0 : 2 * WING + 1] = factor_ref[...]
    back = LANES - 1 - lax.broadcasted_iota(jnp.int32, (SLOTS, LANES), 1)
    pieces = [
        jnp.take_along_axis(
            padded[:, c * LANES : (c + 1) * LANES], back, axis=1, mode="promise_in_bounds"
        )
        for c in (2, 1, 0)
    ]
    factor = jnp.concatenate(pieces, axis=1)
    m = lax.broadcasted_iota(jnp.int32, (SLOTS, REACH), 1)
    offset = (REACH - 1 - WING - m).astype(F32)
    square = offset * offset
    gauss_width = column(gauss_ref[...])
    lorentz_width = column(lorentz_ref[...])
    mixing = column(mixing_ref[...])
    wide = lorentz_width * lorentz_width
    lorentz = wide / (square + wide)
    gauss = jnp.exp(-square / (2.0 * gauss_width * gauss_width))
    raw = (mixing * lorentz + (1.0 - mixing) * gauss) * factor
    raw = jnp.where(m >= REACH - 1 - 2 * WING, raw, 0.0)
    return raw / jnp.sum(raw, axis=1, keepdims=True)


def conv(grid, t_high, t_low):
    rows = grid.shape[0]
    high = grid.astype(BF16).astype(F32)
    both = jnp.concatenate([high, grid - high], axis=0).astype(BF16)
    twice = jnp.dot(both, t_high[...], preferred_element_type=F32)
    rest = jnp.dot(high.astype(BF16), t_low[...], preferred_element_type=F32)
    return twice[0:rows] + twice[rows : 2 * rows] + rest


def kernel(
    n_grp,
    n_dev,
    bin_hbm,
    slot_hbm,
    strength_hbm,
    count_ref,
    gauss_hbm,
    lorentz_hbm,
    mixing_hbm,
    factor_hbm,
    own_ref,
    sum_ref,
    bin_ref,
    slot_ref,
    strength_ref,
    gauss_ref,
    lorentz_ref,
    mixing_ref,
    factor_ref,
    padded,
    t_high,
    t_low,
    wide_ref,
    stage,
    far,
    middle,
    leak_ref,
    near_up,
    near_down,
    lower,
    inbox,
    in_sem,
    send_sem,
    recv_sem,
    relay_sem,
):
    devices = n_grp * n_dev
    dev = lax.axis_index("dev")
    me = lax.axis_index("grp") * n_dev + dev

    loads = [
        pltpu.make_async_copy(source, target, in_sem.at[i])
        for i, (source, target) in enumerate(
            (
                (bin_hbm, bin_ref),
                (slot_hbm, slot_ref),
                (strength_hbm, strength_ref),
                (gauss_hbm, gauss_ref),
                (lorentz_hbm, lorentz_ref),
                (mixing_hbm, mixing_ref),
                (factor_hbm, factor_ref),
            )
        )
    ]
    for load in loads[:3]:
        load.start()
    z = lax.rem(dev, ROW)
    late = z >= ROW // 2

    def exists(o):
        return me + o < devices if o > 0 else me + o >= 0

    def tell(semaphore, condition, o):
        @pl.when(condition)
        def _():
            pl.semaphore_signal(
                semaphore,
                inc=1,
                device_id=(lax.div(me + o, n_dev), lax.rem(me + o, n_dev)),
                device_id_type=pl.DeviceIdType.MESH,
            )

    barrier = pltpu.get_barrier_semaphore()
    crosses = z >= ROW - 2
    heard = ((exists(2) & crosses) | (exists(-2) & (z == 0))).astype(jnp.int32)
    for o in (1, -1):
        heard = heard + exists(o).astype(jnp.int32)
        tell(barrier, exists(-o), -o)
    for load in loads[3:]:
        load.start()
    heard = heard + exists(3).astype(jnp.int32)
    tell(barrier, exists(-3), -3)
    tell(barrier, exists(-2) & (z < 2), -2)
    tell(barrier, exists(2) & (z == ROW - 2), 2)

    padded[...] = jnp.zeros((SLOTS, REACH), F32)
    for index, o in enumerate(OFFSETS):
        @pl.when(jnp.logical_not(exists(-o)))
        def _():
            at, rows = SPOTS[index]
            inbox[at : at + rows, :] = jnp.zeros((rows, LANES), F32)

        if o > 0:

            @pl.when(exists(-o) & (dev == 0))
            def _():
                at, rows = SPOTS[index]
                inbox[at + 1 : at + rows, :] = jnp.zeros((rows - 1, LANES), F32)

    for load in loads[:3]:
        load.wait()

    lines = bin_ref.shape[0] * LANES
    near = bin_ref[...] - (dev - HOP) * SPAN
    slot = slot_ref[...]
    q = near // PART
    wide = (near % PART) * SLOTS + slot
    place = lax.broadcasted_iota(jnp.int32, near.shape, 0) * LANES + lax.broadcasted_iota(
        jnp.int32, near.shape, 1
    )
    weight = jnp.where(place < count_ref[0], strength_ref[...], 0.0)
    weight_high = weight.astype(BF16).astype(F32)
    weight_low = weight - weight_high
    wide = jnp.transpose(wide)
    for load in loads[3:]:
        load.wait()

    lane = lax.broadcasted_iota(jnp.int32, (LANES, LANES), 1)
    spot = lax.broadcasted_iota(jnp.int32, (16, LANES), 0)
    blocks = lines // LANES
    zero = jnp.zeros((16, LANES), BF16)

    def tile_of(value, k, dtype):
        return jnp.broadcast_to(value[k : k + 1, :], (16, LANES)).astype(dtype)

    ahead = n_dev - dev
    pieces = (far.at[pl.ds(16, 8), :], far.at[pl.ds(8, 8), :], near_up)
    pieces += (lower.at[pl.ds(0, 16), :], near_down)

    def copy(index, source=None):
        at, rows = SPOTS[index] if source is None else (SPOTS[index][0], 1)
        o = OFFSETS[index]
        return pltpu.make_async_remote_copy(
            src_ref=pieces[index] if source is None else source,
            dst_ref=inbox.at[pl.ds(at, rows), :],
            send_sem=send_sem.at[index],
            recv_sem=recv_sem.at[index],
            device_id=(lax.div(me + o, n_dev), lax.rem(me + o, n_dev)),
            device_id_type=pl.DeviceIdType.MESH,
        )

    def send(index, condition):
        o = OFFSETS[index]
        condition = jnp.logical_and(exists(o), condition)

        @pl.when(condition & (ahead != o) if o > 0 else condition)
        def _():
            copy(index).start()

    def leak():
        within = near - ((n_dev - dev + HOP) * SPAN - LANES)
        table_high, table_low = split(
            voigt_table(gauss_ref, lorentz_ref, mixing_ref, factor_ref, padded)
        )
        weights, hits = [], []
        for k in range(blocks):
            bin_at = tile_of(within, k, jnp.int16)
            slot_at = tile_of(slot, k, jnp.int16)
            high = tile_of(weight_high, k, BF16)
            low = tile_of(weight_low, k, BF16)
            own = [slot_at == (spot + i * 16).astype(jnp.int16) for i in range(SLOTS // 16)]
            weights.append(
                jnp.concatenate(
                    [jnp.where(hit, part, zero) for part in (high, low) for hit in own], axis=0
                )
            )
            hits.append(
                jnp.concatenate(
                    [
                        jnp.where(
                            bin_at == (spot + i * 16).astype(jnp.int16),
                            jnp.ones((16, LANES), BF16),
                            zero,
                        )
                        for i in range(LANES // 16)
                    ],
                    axis=0,
                )
            )
        hits = jnp.concatenate(hits, axis=1)
        grid = lax.dot_general(
            hits,
            jnp.concatenate(weights, axis=1),
            (((1,), (1,)), ((), ())),
            preferred_element_type=F32,
        )
        high, low = split(grid)
        kernel_high = jnp.concatenate([table_high[:, 2 * LANES :]] * 2, axis=0)
        kernel_low = jnp.concatenate([table_low[:, 2 * LANES :]] * 2, axis=0)
        spread_out = (
            jnp.dot(high, kernel_high, preferred_element_type=F32)
            + jnp.dot(low, kernel_high, preferred_element_type=F32)
            + jnp.dot(high, kernel_low, preferred_element_type=F32)
        )
        moved = pltpu.roll(spread_out, 1, 1, stride=1, stride_axis=0)
        row = lax.broadcasted_iota(jnp.int32, (LANES, LANES), 0)
        return jnp.sum(jnp.where(lane <= row, moved, 0.0), axis=0, keepdims=True)

    edge = (ahead <= 3) & (me + ahead < devices)

    @pl.when(edge)
    def _():
        leak_ref[...] = leak()
        pl.semaphore_wait(barrier, heard)
        for index in range(3):

            @pl.when(ahead == OFFSETS[index])
            def _():
                copy(index, leak_ref).start()

    table = voigt_table(gauss_ref, lorentz_ref, mixing_ref, factor_ref, padded)
    table_high, table_low = split(table)
    for r in range(PART):
        rows = slice(r * SLOTS, (r + 1) * SLOTS)
        t_high[rows, :] = pltpu.roll(table_high, r + 2 * LANES + 1, 1)
        t_low[rows, :] = pltpu.roll(table_low, r + 2 * LANES + 1, 1)

    pairs = wide[:, 0:(blocks // 2)] + wide[:, (blocks // 2) : 2 * (blocks // 2)] * 65536
    wide_ref[...] = pairs

    def unpack(words, k):
        word = words[:, k % (blocks // 2) : k % (blocks // 2) + 1]
        word = jnp.broadcast_to(word, (LANES, LANES))
        return (word if k < (blocks // 2) else word >> 16).astype(jnp.int16)

    def columns(k):
        return unpack(pairs, k)

    def kept(k):
        return unpack(wide_ref[...], k)

    def one_hot(column_of):
        rows = []
        for k in range(blocks):
            at = column_of(k)
            rows.append(
                jnp.concatenate(
                    [
                        jnp.where(
                            at == (lane + c * LANES).astype(jnp.int16),
                            jnp.ones((LANES, LANES), BF16),
                            jnp.zeros((LANES, LANES), BF16),
                        )
                        for c in range(WIDE // LANES)
                    ],
                    axis=1,
                )
            )
        return jnp.concatenate(rows, axis=0)

    def weighted(low_cell, high_cell):
        rows = high_cell - low_cell
        inside = jnp.logical_and(q >= low_cell, q < high_cell)
        place = jnp.where(inside, q - low_cell, -4 * CELLS)
        cols = []
        for k in range(blocks):
            at = tile_of(place, k, jnp.int16)
            at_low = tile_of(place + rows, k, jnp.int16)
            high = tile_of(weight_high, k, BF16)
            low = tile_of(weight_low, k, BF16)
            tiles = []
            for i in range(2 * rows // 16):
                here = (spot + i * 16).astype(jnp.int16)
                value = zero
                if (i + 1) * 16 > rows:
                    value = jnp.where(at_low == here, low, value)
                if i * 16 < rows:
                    value = jnp.where(at == here, high, value)
                tiles.append(value)
            cols.append(jnp.concatenate(tiles, axis=0))
        return jnp.concatenate(cols, axis=1)

    def deposit(low_cell, high_cell, column_of):
        rows = high_cell - low_cell
        both = jnp.dot(
            weighted(low_cell, high_cell), one_hot(column_of), preferred_element_type=F32
        )
        return both[0:rows] + both[rows : 2 * rows]

    def window(total):
        rows = total.shape[0] // SUBS
        for c in range(3):
            stage[c, 0 : total.shape[0], :] = total[:, c * LANES : (c + 1) * LANES]

        def every(sub):
            return jnp.concatenate(
                [stage[c, pl.ds(sub, rows, stride=SUBS), :] for c in range(3)], axis=1
            )

        value = every(0)
        for sub in range(1, SUBS):
            value = value + pltpu.roll(every(sub), sub * PART, 1)
        return value

    def spread(target, at, value):
        rows = value.shape[0]
        target[...] = jnp.zeros(target.shape, F32)
        target[at : at + rows, :] = value[:, 0:LANES]
        target[at + 1 : at + 1 + rows, :] += value[:, LANES : 2 * LANES]
        target[at + 2 : at + 2 + rows, :] += value[:, 2 * LANES : 3 * LANES]

    def greet(condition):
        @pl.when(condition)
        def _():
            pl.semaphore_wait(barrier, heard)

    def pass_on(condition):
        tell(relay_sem.at[0], condition & (z > 0) & (z < ROW - 1), -1)
        tell(relay_sem.at[1], condition & exists(-1) & (z < ROW - 1), 1)

    spread(far, 6, window(conv(deposit(FAR, CELLS, columns), t_high, t_low)))
    greet(late & jnp.logical_not(edge))
    send(0, late)
    send(1, crosses)
    pass_on(late)

    spread(middle, 6, window(conv(deposit(MID, FAR, kept), t_high, t_low)))
    near_up[...] = middle[8:16, :] + far[0:8, :]
    send(2, late)

    spread(lower, 7, window(conv(deposit(0, MID, kept), t_high, t_low)))
    own_ref[...] = lower[24:32, :] + middle[0:8, :]
    def leaks(o):
        return exists(-o) & (dev == 0) if o > 0 else me < 0

    def take(index):
        o = OFFSETS[index]

        @pl.when(exists(-o) & jnp.logical_not(leaks(o)))
        def _():
            copy(index).wait_recv()

        if o > 0:

            @pl.when(leaks(o))
            def _():
                copy(index, leak_ref).wait_recv()

    greet(jnp.logical_not(late))
    send(0, jnp.logical_not(late))
    send(2, jnp.logical_not(late))
    pass_on(jnp.logical_not(late))

    def send_down(condition):
        @pl.when(condition & exists(-2) & (z > 0))
        def _():
            pl.semaphore_wait(relay_sem.at[1], 1)

        send(3, condition)

    send_down(z >= 2)
    take(3)
    near_down[...] = lower[16:24, :] + inbox[24:32, :]
    send(4, True)
    send_down(z < 2)

    @pl.when(jnp.logical_not(crosses))
    def _():
        pl.semaphore_wait(relay_sem.at[0], 1)

    send(1, jnp.logical_not(crosses))
    for index in (4, 2, 1, 0):
        take(index)

    total = inbox[0:8, :]
    for at in (8, 16, 32, 40):
        total = total + inbox[at : at + 8, :]
    sum_ref[...] = total
    for index, o in enumerate(OFFSETS):

        @pl.when(exists(o) & jnp.logical_not(edge & (ahead == o)))
        def _():
            copy(index).wait_send()

        if o > 0:

            @pl.when(edge & (ahead == o))
            def _():
                copy(index, leak_ref).wait_send()


def solution(mesh):
    n_grp, n_dev = mesh.shape["grp"], mesh.shape["dev"]

    def body(
        line_bin, line_slot, strength, line_count, gauss_width, lorentz_width, mixing, factor
    ):
        lines = line_bin.shape[0]

        def call(*refs):
            kernel(n_grp, n_dev, *refs)

        vmem = pl.BlockSpec(memory_space=pltpu.VMEM)
        hbm = pl.BlockSpec(memory_space=pltpu.HBM)
        piece = jax.ShapeDtypeStruct((SPAN // LANES, LANES), F32)
        own, received = pl.pallas_call(
            call,
            out_shape=(piece, piece),
            in_specs=[hbm] * 3 + [pl.BlockSpec(memory_space=pltpu.SMEM)] + [hbm] * 4,
            out_specs=(vmem, vmem),
            scratch_shapes=[
                pltpu.VMEM((lines // LANES, LANES), jnp.int32),
                pltpu.VMEM((lines // LANES, LANES), jnp.int32),
                pltpu.VMEM((lines // LANES, LANES), F32),
                pltpu.VMEM((1, SLOTS), F32),
                pltpu.VMEM((1, SLOTS), F32),
                pltpu.VMEM((1, SLOTS), F32),
                pltpu.VMEM((SLOTS, 2 * WING + 1), F32),
                pltpu.VMEM((SLOTS, REACH), F32),
                pltpu.VMEM((WIDE, REACH), BF16),
                pltpu.VMEM((WIDE, REACH), BF16),
                pltpu.VMEM((LANES, lines // LANES // 2), jnp.int32),
                pltpu.VMEM((3, MID, LANES), F32),
                pltpu.VMEM((3 * 8, LANES), F32),
                pltpu.VMEM((2 * 8, LANES), F32),
                pltpu.VMEM((1, LANES), F32),
                pltpu.VMEM((8, LANES), F32),
                pltpu.VMEM((8, LANES), F32),
                pltpu.VMEM((4 * 8, LANES), F32),
                pltpu.VMEM((6 * 8, LANES), F32),
                pltpu.SemaphoreType.DMA((7,)),
                pltpu.SemaphoreType.DMA((5,)),
                pltpu.SemaphoreType.DMA((5,)),
                pltpu.SemaphoreType.REGULAR((2,)),
            ],
            compiler_params=pltpu.CompilerParams(
                collective_id=0,
                has_side_effects=True,
                vmem_limit_bytes=GRANT,
            ),
            name="voigt",
        )(
            *(
                value if value.size == 1 else pltpu.with_memory_space_constraint(value, pltpu.HBM)
                for value in (
                    line_bin.reshape(lines // LANES, LANES),
                    line_slot.reshape(lines // LANES, LANES),
                    strength.reshape(lines // LANES, LANES),
                    line_count,
                    gauss_width.reshape(1, SLOTS),
                    lorentz_width.reshape(1, SLOTS),
                    mixing.reshape(1, SLOTS),
                    factor,
                )
            )
        )
        return (own + received).reshape(SPAN)

    split_over = P(("grp", "dev"))
    return jax.shard_map(
        body,
        mesh=mesh,
        in_specs=(split_over,) * 4 + (P(),) * 4,
        out_specs=split_over,
        check_vma=False,
    )
```

```python
import jax
import jax.numpy as jnp
from jax import lax
from jax.experimental import pallas as pl
from jax.experimental.pallas import tpu as pltpu
from jax.sharding import PartitionSpec as P

SLOTS = 32
WING = 128
HOP = 2
SPAN = 1024
LANES = 128
ROW = 16
OFFSETS = (3, 2, 1, -2, -1)
SPOTS = ((0, 8), (8, 8), (16, 8), (24, 16), (40, 8))
BF16 = jnp.bfloat16
F32 = jnp.float32
ROWS = (2 * HOP + 1) * SPAN // LANES
PART = 16
SUBS = LANES // PART
WIDE = PART * SLOTS
REACH = 3 * LANES
CELLS = SUBS * ROWS
FAR = 248
MID = 184


GRANT = 24 << 20


def split(value):
    high = value.astype(BF16)
    low = (value - high.astype(F32)).astype(BF16)
    return high, low


def column(row):
    i = lax.broadcasted_iota(jnp.int32, (SLOTS, SLOTS), 0)
    j = lax.broadcasted_iota(jnp.int32, (SLOTS, SLOTS), 1)
    spread = jnp.where(i == j, jnp.broadcast_to(row, (SLOTS, SLOTS)), 0.0)
    return jnp.sum(spread, axis=1, keepdims=True)


def voigt_table(gauss_ref, lorentz_ref, mixing_ref, factor_ref, padded):
    padded[:, 0 : 2 * WING + 1] = factor_ref[...]
    back = LANES - 1 - lax.broadcasted_iota(jnp.int32, (SLOTS, LANES), 1)
    pieces = [
        jnp.take_along_axis(
            padded[:, c * LANES : (c + 1) * LANES], back, axis=1, mode="promise_in_bounds"
        )
        for c in (2, 1, 0)
    ]
    factor = jnp.concatenate(pieces, axis=1)
    m = lax.broadcasted_iota(jnp.int32, (SLOTS, REACH), 1)
    offset = (REACH - 1 - WING - m).astype(F32)
    square = offset * offset
    gauss_width = column(gauss_ref[...])
    lorentz_width = column(lorentz_ref[...])
    mixing = column(mixing_ref[...])
    wide = lorentz_width * lorentz_width
    lorentz = wide / (square + wide)
    gauss = jnp.exp(-square / (2.0 * gauss_width * gauss_width))
    raw = (mixing * lorentz + (1.0 - mixing) * gauss) * factor
    raw = jnp.where(m >= REACH - 1 - 2 * WING, raw, 0.0)
    return raw / jnp.sum(raw, axis=1, keepdims=True)


def conv(grid, t_high, t_low):
    rows = grid.shape[0]
    high = grid.astype(BF16).astype(F32)
    both = jnp.concatenate([high, grid - high], axis=0).astype(BF16)
    twice = jnp.dot(both, t_high[...], preferred_element_type=F32)
    rest = jnp.dot(high.astype(BF16), t_low[...], preferred_element_type=F32)
    return twice[0:rows] + twice[rows : 2 * rows] + rest


def kernel(
    n_grp,
    n_dev,
    bin_hbm,
    slot_hbm,
    strength_hbm,
    count_ref,
    gauss_hbm,
    lorentz_hbm,
    mixing_hbm,
    factor_hbm,
    own_ref,
    sum_ref,
    bin_ref,
    slot_ref,
    strength_ref,
    gauss_ref,
    lorentz_ref,
    mixing_ref,
    factor_ref,
    padded,
    t_high,
    t_low,
    wide_ref,
    stage,
    far,
    middle,
    leak_ref,
    near_up,
    near_down,
    lower,
    inbox,
    in_sem,
    send_sem,
    recv_sem,
    relay_sem,
):
    devices = n_grp * n_dev
    dev = lax.axis_index("dev")
    me = lax.axis_index("grp") * n_dev + dev

    loads = [
        pltpu.make_async_copy(source, target, in_sem.at[i])
        for i, (source, target) in enumerate(
            (
                (bin_hbm, bin_ref),
                (slot_hbm, slot_ref),
                (strength_hbm, strength_ref),
                (gauss_hbm, gauss_ref),
                (lorentz_hbm, lorentz_ref),
                (mixing_hbm, mixing_ref),
                (factor_hbm, factor_ref),
            )
        )
    ]
    for load in loads[:3] + loads[6:]:
        load.start()
    z = lax.rem(dev, ROW)
    late = z >= ROW // 2

    def exists(o):
        return me + o < devices if o > 0 else me + o >= 0

    def tell(semaphore, condition, o):
        @pl.when(condition)
        def _():
            pl.semaphore_signal(
                semaphore,
                inc=1,
                device_id=(lax.div(me + o, n_dev), lax.rem(me + o, n_dev)),
                device_id_type=pl.DeviceIdType.MESH,
            )

    barrier = pltpu.get_barrier_semaphore()
    crosses = z >= ROW - 2
    heard = ((exists(2) & crosses) | (exists(-2) & (z == 0))).astype(jnp.int32)
    for o in (1, -1):
        heard = heard + exists(o).astype(jnp.int32)
        tell(barrier, exists(-o), -o)
    for load in loads[3:6]:
        load.start()
    heard = heard + exists(3).astype(jnp.int32)
    tell(barrier, exists(-3), -3)
    tell(barrier, exists(-2) & (z < 2), -2)
    tell(barrier, exists(2) & (z == ROW - 2), 2)

    padded[...] = jnp.zeros((SLOTS, REACH), F32)
    for index, o in enumerate(OFFSETS):
        @pl.when(jnp.logical_not(exists(-o)))
        def _():
            at, rows = SPOTS[index]
            inbox[at : at + rows, :] = jnp.zeros((rows, LANES), F32)

        if o > 0:

            @pl.when(exists(-o) & (dev == 0))
            def _():
                at, rows = SPOTS[index]
                inbox[at + 1 : at + rows, :] = jnp.zeros((rows - 1, LANES), F32)

    for load in loads[:3]:
        load.wait()

    lines = bin_ref.shape[0] * LANES
    near = bin_ref[...] - (dev - HOP) * SPAN
    slot = slot_ref[...]
    q = near // PART
    wide = (near % PART) * SLOTS + slot
    place = lax.broadcasted_iota(jnp.int32, near.shape, 0) * LANES + lax.broadcasted_iota(
        jnp.int32, near.shape, 1
    )
    weight = jnp.where(place < count_ref[0], strength_ref[...], 0.0)
    weight_high = weight.astype(BF16).astype(F32)
    weight_low = weight - weight_high
    wide = jnp.transpose(wide)
    for load in loads[3:]:
        load.wait()

    lane = lax.broadcasted_iota(jnp.int32, (LANES, LANES), 1)
    spot = lax.broadcasted_iota(jnp.int32, (16, LANES), 0)
    blocks = lines // LANES
    zero = jnp.zeros((16, LANES), BF16)

    def tile_of(value, k, dtype):
        return jnp.broadcast_to(value[k : k + 1, :], (16, LANES)).astype(dtype)

    ahead = n_dev - dev
    pieces = (far.at[pl.ds(16, 8), :], far.at[pl.ds(8, 8), :], near_up)
    pieces += (lower.at[pl.ds(0, 16), :], near_down)

    def copy(index, source=None):
        at, rows = SPOTS[index] if source is None else (SPOTS[index][0], 1)
        o = OFFSETS[index]
        return pltpu.make_async_remote_copy(
            src_ref=pieces[index] if source is None else source,
            dst_ref=inbox.at[pl.ds(at, rows), :],
            send_sem=send_sem.at[index],
            recv_sem=recv_sem.at[index],
            device_id=(lax.div(me + o, n_dev), lax.rem(me + o, n_dev)),
            device_id_type=pl.DeviceIdType.MESH,
        )

    def send(index, condition):
        o = OFFSETS[index]
        condition = jnp.logical_and(exists(o), condition)

        @pl.when(condition & (ahead != o) if o > 0 else condition)
        def _():
            copy(index).start()

    def leak():
        within = near - ((n_dev - dev + HOP) * SPAN - LANES)
        table_high, table_low = split(
            voigt_table(gauss_ref, lorentz_ref, mixing_ref, factor_ref, padded)
        )
        weights, hits = [], []
        for k in range(blocks):
            bin_at = tile_of(within, k, jnp.int16)
            slot_at = tile_of(slot, k, jnp.int16)
            high = tile_of(weight_high, k, BF16)
            low = tile_of(weight_low, k, BF16)
            own = [slot_at == (spot + i * 16).astype(jnp.int16) for i in range(SLOTS // 16)]
            weights.append(
                jnp.concatenate(
                    [jnp.where(hit, part, zero) for part in (high, low) for hit in own], axis=0
                )
            )
            hits.append(
                jnp.concatenate(
                    [
                        jnp.where(
                            bin_at == (spot + i * 16).astype(jnp.int16),
                            jnp.ones((16, LANES), BF16),
                            zero,
                        )
                        for i in range(LANES // 16)
                    ],
                    axis=0,
                )
            )
        hits = jnp.concatenate(hits, axis=1)
        grid = lax.dot_general(
            hits,
            jnp.concatenate(weights, axis=1),
            (((1,), (1,)), ((), ())),
            preferred_element_type=F32,
        )
        high, low = split(grid)
        kernel_high = jnp.concatenate([table_high[:, 2 * LANES :]] * 2, axis=0)
        kernel_low = jnp.concatenate([table_low[:, 2 * LANES :]] * 2, axis=0)
        spread_out = (
            jnp.dot(high, kernel_high, preferred_element_type=F32)
            + jnp.dot(low, kernel_high, preferred_element_type=F32)
            + jnp.dot(high, kernel_low, preferred_element_type=F32)
        )
        moved = pltpu.roll(spread_out, 1, 1, stride=1, stride_axis=0)
        row = lax.broadcasted_iota(jnp.int32, (LANES, LANES), 0)
        return jnp.sum(jnp.where(lane <= row, moved, 0.0), axis=0, keepdims=True)

    edge = (ahead <= 3) & (me + ahead < devices)

    @pl.when(edge)
    def _():
        leak_ref[...] = leak()
        pl.semaphore_wait(barrier, heard)
        for index in range(3):

            @pl.when(ahead == OFFSETS[index])
            def _():
                copy(index, leak_ref).start()

    table = voigt_table(gauss_ref, lorentz_ref, mixing_ref, factor_ref, padded)
    table_high, table_low = split(table)
    for r in range(PART):
        rows = slice(r * SLOTS, (r + 1) * SLOTS)
        t_high[rows, :] = pltpu.roll(table_high, r + 2 * LANES + 1, 1)
        t_low[rows, :] = pltpu.roll(table_low, r + 2 * LANES + 1, 1)

    pairs = wide[:, 0:(blocks // 2)] + wide[:, (blocks // 2) : 2 * (blocks // 2)] * 65536
    wide_ref[...] = pairs

    def unpack(words, k):
        word = words[:, k % (blocks // 2) : k % (blocks // 2) + 1]
        word = jnp.broadcast_to(word, (LANES, LANES))
        return (word if k < (blocks // 2) else word >> 16).astype(jnp.int16)

    def columns(k):
        return unpack(pairs, k)

    def kept(k):
        return unpack(wide_ref[...], k)

    def one_hot(column_of):
        rows = []
        for k in range(blocks):
            at = column_of(k)
            rows.append(
                jnp.concatenate(
                    [
                        jnp.where(
                            at == (lane + c * LANES).astype(jnp.int16),
                            jnp.ones((LANES, LANES), BF16),
                            jnp.zeros((LANES, LANES), BF16),
                        )
                        for c in range(WIDE // LANES)
                    ],
                    axis=1,
                )
            )
        return jnp.concatenate(rows, axis=0)

    def weighted(low_cell, high_cell):
        rows = high_cell - low_cell
        inside = jnp.logical_and(q >= low_cell, q < high_cell)
        place = jnp.where(inside, q - low_cell, -4 * CELLS)
        cols = []
        for k in range(blocks):
            at = tile_of(place, k, jnp.int16)
            at_low = tile_of(place + rows, k, jnp.int16)
            high = tile_of(weight_high, k, BF16)
            low = tile_of(weight_low, k, BF16)
            tiles = []
            for i in range(2 * rows // 16):
                here = (spot + i * 16).astype(jnp.int16)
                value = zero
                if (i + 1) * 16 > rows:
                    value = jnp.where(at_low == here, low, value)
                if i * 16 < rows:
                    value = jnp.where(at == here, high, value)
                tiles.append(value)
            cols.append(jnp.concatenate(tiles, axis=0))
        return jnp.concatenate(cols, axis=1)

    def deposit(low_cell, high_cell, column_of):
        rows = high_cell - low_cell
        both = jnp.dot(
            weighted(low_cell, high_cell), one_hot(column_of), preferred_element_type=F32
        )
        return both[0:rows] + both[rows : 2 * rows]

    def window(total):
        rows = total.shape[0] // SUBS
        for c in range(3):
            stage[c, 0 : total.shape[0], :] = total[:, c * LANES : (c + 1) * LANES]

        def every(sub):
            return jnp.concatenate(
                [stage[c, pl.ds(sub, rows, stride=SUBS), :] for c in range(3)], axis=1
            )

        value = every(0)
        for sub in range(1, SUBS):
            value = value + pltpu.roll(every(sub), sub * PART, 1)
        return value

    def spread(target, at, value):
        rows = value.shape[0]
        target[...] = jnp.zeros(target.shape, F32)
        target[at : at + rows, :] = value[:, 0:LANES]
        target[at + 1 : at + 1 + rows, :] += value[:, LANES : 2 * LANES]
        target[at + 2 : at + 2 + rows, :] += value[:, 2 * LANES : 3 * LANES]

    def greet(condition):
        @pl.when(condition)
        def _():
            pl.semaphore_wait(barrier, heard)

    def pass_on(condition):
        tell(relay_sem.at[0], condition & (z > 0) & (z < ROW - 1), -1)
        tell(relay_sem.at[1], condition & exists(-1) & (z < ROW - 1), 1)

    spread(far, 6, window(conv(deposit(FAR, CELLS, columns), t_high, t_low)))
    greet(late & jnp.logical_not(edge))
    send(0, late)
    send(1, crosses)
    pass_on(late)

    spread(middle, 6, window(conv(deposit(MID, FAR, kept), t_high, t_low)))
    near_up[...] = middle[8:16, :] + far[0:8, :]
    send(2, late)

    spread(lower, 7, window(conv(deposit(0, MID, kept), t_high, t_low)))
    own_ref[...] = lower[24:32, :] + middle[0:8, :]
    def leaks(o):
        return exists(-o) & (dev == 0) if o > 0 else me < 0

    def take(index):
        o = OFFSETS[index]

        @pl.when(exists(-o) & jnp.logical_not(leaks(o)))
        def _():
            copy(index).wait_recv()

        if o > 0:

            @pl.when(leaks(o))
            def _():
                copy(index, leak_ref).wait_recv()

    greet(jnp.logical_not(late))
    send(0, jnp.logical_not(late))
    send(2, jnp.logical_not(late))
    pass_on(jnp.logical_not(late))

    def send_down(condition):
        @pl.when(condition & exists(-2) & (z > 0))
        def _():
            pl.semaphore_wait(relay_sem.at[1], 1)

        send(3, condition)

    send_down(z >= 2)
    take(3)
    near_down[...] = lower[16:24, :] + inbox[24:32, :]
    send(4, True)
    send_down(z < 2)

    @pl.when(jnp.logical_not(crosses))
    def _():
        pl.semaphore_wait(relay_sem.at[0], 1)

    send(1, jnp.logical_not(crosses))
    for index in (4, 2, 1, 0):
        take(index)

    total = inbox[0:8, :]
    for at in (8, 16, 32, 40):
        total = total + inbox[at : at + 8, :]
    sum_ref[...] = total
    for index, o in enumerate(OFFSETS):

        @pl.when(exists(o) & jnp.logical_not(edge & (ahead == o)))
        def _():
            copy(index).wait_send()

        if o > 0:

            @pl.when(edge & (ahead == o))
            def _():
                copy(index, leak_ref).wait_send()


def solution(mesh):
    n_grp, n_dev = mesh.shape["grp"], mesh.shape["dev"]

    def body(
        line_bin, line_slot, strength, line_count, gauss_width, lorentz_width, mixing, factor
    ):
        lines = line_bin.shape[0]

        def call(*refs):
            kernel(n_grp, n_dev, *refs)

        vmem = pl.BlockSpec(memory_space=pltpu.VMEM)
        hbm = pl.BlockSpec(memory_space=pltpu.HBM)
        piece = jax.ShapeDtypeStruct((SPAN // LANES, LANES), F32)
        own, received = pl.pallas_call(
            call,
            out_shape=(piece, piece),
            in_specs=[hbm] * 3 + [pl.BlockSpec(memory_space=pltpu.SMEM)] + [hbm] * 4,
            out_specs=(vmem, vmem),
            scratch_shapes=[
                pltpu.VMEM((lines // LANES, LANES), jnp.int32),
                pltpu.VMEM((lines // LANES, LANES), jnp.int32),
                pltpu.VMEM((lines // LANES, LANES), F32),
                pltpu.VMEM((1, SLOTS), F32),
                pltpu.VMEM((1, SLOTS), F32),
                pltpu.VMEM((1, SLOTS), F32),
                pltpu.VMEM((SLOTS, 2 * WING + 1), F32),
                pltpu.VMEM((SLOTS, REACH), F32),
                pltpu.VMEM((WIDE, REACH), BF16),
                pltpu.VMEM((WIDE, REACH), BF16),
                pltpu.VMEM((LANES, lines // LANES // 2), jnp.int32),
                pltpu.VMEM((3, MID, LANES), F32),
                pltpu.VMEM((3 * 8, LANES), F32),
                pltpu.VMEM((2 * 8, LANES), F32),
                pltpu.VMEM((1, LANES), F32),
                pltpu.VMEM((8, LANES), F32),
                pltpu.VMEM((8, LANES), F32),
                pltpu.VMEM((4 * 8, LANES), F32),
                pltpu.VMEM((6 * 8, LANES), F32),
                pltpu.SemaphoreType.DMA((7,)),
                pltpu.SemaphoreType.DMA((5,)),
                pltpu.SemaphoreType.DMA((5,)),
                pltpu.SemaphoreType.REGULAR((2,)),
            ],
            compiler_params=pltpu.CompilerParams(
                collective_id=0,
                has_side_effects=True,
                vmem_limit_bytes=GRANT,
            ),
            name="voigt",
        )(
            *(
                value if value.size == 1 else pltpu.with_memory_space_constraint(value, pltpu.HBM)
                for value in (
                    line_bin.reshape(lines // LANES, LANES),
                    line_slot.reshape(lines // LANES, LANES),
                    strength.reshape(lines // LANES, LANES),
                    line_count,
                    gauss_width.reshape(1, SLOTS),
                    lorentz_width.reshape(1, SLOTS),
                    mixing.reshape(1, SLOTS),
                    factor,
                )
            )
        )
        return (own + received).reshape(SPAN)

    split_over = P(("grp", "dev"))
    return jax.shard_map(
        body,
        mesh=mesh,
        in_specs=(split_over,) * 4 + (P(),) * 4,
        out_specs=split_over,
        check_vma=False,
    )
```
